32 devices in a mesh: rep: 1 (over z), dp: 32 (over x, y, core).
Axes of the slice: x: 4, y: 4, z: 1, core: 2. Of those that a mesh axis runs over, the one named last changes fastest.
The devices are a block of a 4x4x8 slice.
Arguments:
- g_w_gate: bfloat16 [32, 2, 512, 4096], P(('rep', 'dp'))
- g_w_up: bfloat16 [32, 2, 512, 4096], P(('rep', 'dp'))
- g_w_down: bfloat16 [32, 2, 4096, 512], P(('rep', 'dp'))
- w_gate: bfloat16 [2, 512, 4096], replicated
- w_up: bfloat16 [2, 512, 4096], replicated
- w_down: bfloat16 [2, 4096, 512], replicated
- m_w_gate: float32 [2, 512, 4096], P(None, 'dp')
- m_w_up: float32 [2, 512, 4096], P(None, 'dp')
- m_w_down: float32 [2, 4096, 512], P(None, 'dp')
- v_w_gate: float32 [2, 512, 4096], P(None, 'dp')
- v_w_up: float32 [2, 512, 4096], P(None, 'dp')
- v_w_down: float32 [2, 4096, 512], P(None, 'dp')
Outputs:
- output 1: bfloat16 [2, 512, 4096], P('rep')
- output 2: bfloat16 [2, 512, 4096], P('rep')
- output 3: bfloat16 [2, 4096, 512], P('rep')
- output 4: float32 [2, 512, 4096], P('rep', 'dp')
- output 5: float32 [2, 512, 4096], P('rep', 'dp')
- output 6: float32 [2, 4096, 512], P('rep', 'dp')
- output 7: float32 [2, 512, 4096], P('rep', 'dp')
- output 8: float32 [2, 512, 4096], P('rep', 'dp')
- output 9: float32 [2, 4096, 512], P('rep', 'dp')
All inputs are finite; a program needn't handle non-finite values.
Results may differ from the reference program's by a relative error of at most 0.022.
Values are sent between devices in bfloat16 or wider.
A program may use at most 768 MiB of HBM per device.

```python
import jax
import jax.numpy as jnp
from jax import lax

DEVICES = 32
D = 512
FF = 4096
LAYERS = 2
NAMES = ("w_gate", "w_up", "w_down")
SHAPES = {"w_gate": (LAYERS, D, FF), "w_up": (LAYERS, D, FF), "w_down": (LAYERS, FF, D)}


def setup_inputs(seed: int = 0, part: int = 0) -> dict:
    kz, *keys = jax.random.split(jax.random.key(seed), 1 + 5 * len(NAMES))
    loud = 2.0 ** jax.random.uniform(kz, (), jnp.float32, -1.0, 1.0)
    drawn = {}
    for name, key, both in zip(NAMES, keys[:3], keys[3:6], strict=True):
        own = jax.random.normal(jax.random.fold_in(key, part), (DEVICES, *SHAPES[name]), jnp.float32)
        shared = jax.random.normal(jax.random.fold_in(both, part), SHAPES[name], jnp.float32)
        drawn["g_" + name] = (loud * (0.7 * shared / DEVICES + 0.7 * own * DEVICES**-0.5)).astype(jnp.bfloat16)
    for name, key in zip(NAMES, keys[6:9], strict=True):
        drawn[name] = (jax.random.normal(key, SHAPES[name], jnp.float32) * SHAPES[name][1] ** -0.5).astype(jnp.bfloat16)
    for name, key in zip(NAMES, keys[9:12], strict=True):
        drawn["m_" + name] = loud * 0.5 * jax.random.normal(key, SHAPES[name], jnp.float32)
    for name, key in zip(NAMES, keys[12:15], strict=True):
        drawn["v_" + name] = loud * loud * jax.random.uniform(key, SHAPES[name], jnp.float32, 0.5, 1.5)
    return drawn


def adamw(w, m, v, g):
    m = 0.9 * m + 0.1 * g
    v = 0.95 * v + 0.05 * g * g
    step = m * lax.rsqrt(v + 1e-8) + 0.1 * w
    return (w - 0.02 * step).astype(jnp.bfloat16), m, v


def clipped(gradients, sum_of_squares, count):
    factor = jnp.minimum(1.0, 0.5 * lax.rsqrt(sum_of_squares / count + 1e-30))
    return [g * factor for g in gradients]


def reference(g_w_gate, g_w_up, g_w_down, w_gate, w_up, w_down, m_w_gate, m_w_up, m_w_down, v_w_gate, v_w_up, v_w_down):
    def total(terms):
        return lax.scan(lambda so_far, term: (so_far + term.astype(jnp.float32), None), jnp.zeros(terms.shape[1:], jnp.float32), terms)[0]

    gradients = [total(terms).astype(jnp.bfloat16).astype(jnp.float32) for terms in (g_w_gate, g_w_up, g_w_down)]
    gradients = clipped(gradients, sum(jnp.sum(g * g) for g in gradients), sum(g.size for g in gradients))
    new = [
        adamw(w.astype(jnp.float32), m, v, g)
        for w, m, v, g in zip((w_gate, w_up, w_down), (m_w_gate, m_w_up, m_w_down), (v_w_gate, v_w_up, v_w_down), gradients, strict=True)
    ]
    return tuple(one[which] for which in range(3) for one in new)
```

```python
import functools
import math

import jax
import jax.numpy as jnp
from jax import lax
from jax.experimental import pallas as pl
from jax.experimental.pallas import tpu as pltpu
from jax.sharding import PartitionSpec as P

CORES = 2
ROWS, COLS = 16, 512


def strips(shape):
    rows, cols = shape
    if rows > ROWS:
        return rows // ROWS, lambda i: (pl.ds(pl.multiple_of(i * ROWS, ROWS), ROWS), slice(None))
    return cols // COLS, lambda i: (slice(None), pl.ds(pl.multiple_of(i * COLS, COLS), COLS))


def kernel(n, side, *refs):
    (t, w, m, v, o, mo, vo, ring, pair, kept, g, held) = (refs[3 * i : 3 * i + 3] for i in range(12))
    (
        parts, own_sem, mate_sem, ring_sem, pair_sem, part_sem, state_sem, back_sem,
        mate_out, ring_out, pair_out, part_out,
    ) = refs[36:]
    kinds, layers = range(3), range(2)
    f32, bf16 = jnp.float32, jnp.bfloat16

    me = lax.axis_index("dp")
    core, chip = lax.rem(me, CORES), lax.div(me, CORES)
    x, y = lax.div(chip, side), lax.rem(chip, side)
    a, b = x + core * (y - x), y + core * (x - y)
    mate = {"dp": me + 1 - 2 * core}

    def turn(i):
        return lax.rem(i + side, side)

    def place(a_, b_, core_=core):
        return a_ + core_ * (b_ - a_), b_ + core_ * (a_ - b_)

    def device(a_, b_):
        x_, y_ = place(a_, b_)
        return {"dp": (x_ * side + y_) * CORES + core}

    near_a = [device(turn(a + 1), b), device(turn(a - 1), b)]
    near_b = [device(a, turn(b + 1)), device(a, turn(b - 1))]

    def off(k):
        return 2 + k - 3 * (k // 2) - 2 * (k // 3)

    def role(d, s, k, a_, b_):
        step = 1 - 2 * d
        to = turn(a_ + (0 if s == 3 else step + step * (s == 0)))
        return (1 - d if s == 1 else d), to, turn(b_ + off(k))

    def block(j, layer, a_, b_):
        return o[j].at[(layer, *place(a_, b_), core)]

    def other(j, layer, a_, b_):
        return o[j].at[(layer, *place(a_, b_), 1 - core)]

    def load(s, k):
        for d in layers:
            layer, a_, b_ = role(d, s, k, a, b)
            for j in kinds:
                pltpu.make_async_copy(t[j].at[(layer, *place(a_, b_), core)], block(j, layer, a_, b_), own_sem.at[d, s, k, j]).start()

    def hand(s, k):
        for d in layers:
            layer, a_, b_ = role(d, s, k, b, a)
            at = place(a_, b_, 1 - core)
            for j in kinds:
                pltpu.make_async_remote_copy(
                    t[j].at[(layer, *at, 1 - core)], o[j].at[(layer, *at, core)], mate_out.at[j], mate_sem.at[d, s, k, j], device_id=mate
                ).start()

    def arrived(ref, sem):
        pltpu.make_async_copy(ref, ref, sem).wait()

    def send(src, dst, out_sem, sem, to):
        pltpu.make_async_remote_copy(src, dst, out_sem, sem, device_id=to).start()

    def total(j, d, s, k, more=(), into=None):
        layer, a_, b_ = role(d, s, k, a, b)
        mine, its = block(j, layer, a_, b_), other(j, layer, a_, b_)
        into = mine if into is None else into
        arrived(mine, own_sem.at[d, s, k, j])
        arrived(its, mate_sem.at[d, s, k, j])
        count, cut = strips(mine.shape)

        @pl.loop(0, count)
        def _(i):
            at = cut(i)
            so_far = mine[at].astype(f32) + its[at].astype(f32)
            for one in more:
                so_far += one[at].astype(f32)
            into[at] = so_far.astype(into.dtype)

        return mine

    for j in kinds:
        x_, y_ = place(a, b)
        pltpu.make_async_copy(w[j].at[:, x_, y_, core], held[j], state_sem.at[0, j]).start()

    @pl.loop(0, side)
    def _(k):
        load(0, k)

    barrier = pltpu.get_barrier_semaphore()
    for to in (*near_a, *near_b, mate):
        pl.semaphore_signal(barrier, inc=1, device_id=to)
    pl.semaphore_wait(barrier, 5)

    @pl.loop(0, side)
    def _(k):
        hand(0, k)

    for s in (1, 2, 3):
        pl.loop(0, side)(functools.partial(load, s))
    for j in kinds:
        pltpu.make_async_copy(m[j], mo[j], state_sem.at[1, j]).start()
        pltpu.make_async_copy(v[j], vo[j], state_sem.at[2, j]).start()

    for s in range(3):

        @pl.loop(0, side)
        def _(k, s=s):
            hand(s + 1, k)
            for j in kinds:
                for d in layers:
                    more = ()
                    if s == 2:
                        arrived(ring[j].at[d, 0, k], ring_sem.at[d, 0, k, j])
                        more = (ring[j].at[d, 0, k],)
                    mine = total(j, d, s, k, more)
                    send(mine, ring[j].at[d, s, k], ring_out.at[j], ring_sem.at[d, s, k, j], near_a[d])

    def last(j, layer, k, more=(), into=None):
        came = [ring[j].at[layer, 2, k], ring[j].at[1 - layer, 1, k]]
        arrived(came[0], ring_sem.at[layer, 2, k, j])
        arrived(came[1], ring_sem.at[1 - layer, 1, k, j])
        return total(j, layer, 3, k, (*came, *more), into)

    def onward(j, layer, k, d, s, more=()):
        send(last(j, layer, k, more), pair[j].at[d, s], pair_out.at[j], pair_sem.at[d, s, j], near_b[d])

    for j in kinds:
        for d in layers:
            onward(j, d, 0, d, 0)
    for j in kinds:
        onward(j, 0, 1, 1, 1)
        onward(j, 1, 2, 0, 1)
    for j in kinds:
        for layer, k, d in ((1, 1, 1), (0, 2, 0)):
            arrived(pair[j].at[d, 0], pair_sem.at[d, 0, j])
            onward(j, layer, k, d, 2, (pair[j].at[d, 0],))
    for j in kinds:
        for layer in layers:
            last(j, layer, 3, into=kept[j].at[layer])

    squares = jnp.zeros((ROWS, COLS), f32)
    for j in kinds:
        for layer in layers:
            came = [pair[j].at[layer, 2], pair[j].at[1 - layer, 1]]
            arrived(came[0], pair_sem.at[layer, 2, j])
            arrived(came[1], pair_sem.at[1 - layer, 1, j])
            count, cut = strips(came[0].shape)

            def finish(i, so_far, j=j, layer=layer, came=came, cut=cut):
                at = cut(i)
                grad = kept[j].at[layer][at] + came[0][at].astype(f32) + came[1][at].astype(f32)
                grad = grad.astype(bf16)
                g[j].at[layer][at] = grad
                grad = grad.astype(f32)
                return so_far + grad * grad

            squares = lax.fori_loop(0, count, finish, squares)
    by_lane = jnp.sum(squares, axis=0, keepdims=True)
    parts[me] = sum(by_lane[:, i * 128 : (i + 1) * 128] for i in range(COLS // 128))
    for j in kinds:
        arrived(ring[j], ring_out.at[j])
        arrived(pair[j], pair_out.at[j])
        arrived(o[j].at[:, :, :, 0], mate_out.at[j])

    @pl.loop(1, n)
    def _(i):
        send(parts.at[me], parts.at[me], part_out, part_sem, {"dp": lax.rem(me + i, n)})

    for j in kinds:
        arrived(held[j], state_sem.at[0, j])
        arrived(mo[j], state_sem.at[1, j])
        arrived(vo[j], state_sem.at[2, j])
    arrived(parts.at[pl.ds(0, n - 1)], part_sem)
    count = n * sum(math.prod(one.shape) for one in mo)
    whole = jnp.sum(jnp.sum(parts[...], axis=0), axis=1, keepdims=True)
    factor = jnp.minimum(1.0, 0.5 * lax.rsqrt(whole / count + 1e-30))

    def pass_on(j, layer, a_, b_, *, along_a=(), along_b=()):
        one = block(j, layer, a_, b_)
        for d, s in along_b:
            send(one, one, pair_out.at[j], pair_sem.at[d, s, j], near_b[d])
        for d, s, k in along_a:
            send(one, one, ring_out.at[j], ring_sem.at[d, s, k, j], near_a[d])
        send(one, one, mate_out.at[j], back_sem.at[j], mate)

    for layer in layers:
        for j in kinds:
            new = block(j, layer, a, b)
            count, cut = strips(new.shape)

            @pl.loop(0, count)
            def _(i, j=j, layer=layer, new=new, cut=cut):
                at = cut(i)
                grad = g[j].at[layer][at].astype(f32) * factor
                m_ = 0.9 * mo[j].at[layer][at] + 0.1 * grad
                v_ = 0.95 * vo[j].at[layer][at] + 0.05 * grad * grad
                w_ = held[j].at[layer][at].astype(f32)
                mo[j].at[layer][at] = m_
                vo[j].at[layer][at] = v_
                new[at] = (w_ - 0.02 * (m_ * lax.rsqrt(v_ + 1e-8) + 0.1 * w_)).astype(bf16)

            pass_on(j, layer, a, b, along_a=[(d, layer, 3) for d in layers], along_b=[(d, layer) for d in layers])

    def from_b(j, d, s):
        layer = d if s == 2 else s
        step = 1 - 2 * d
        b_ = turn(b - (2 if s == 2 else 1) * step)
        k = 0 if s == 2 else 1 + d
        arrived(block(j, layer, a, b_), pair_sem.at[d, s, j])
        pass_on(j, layer, a, b_, along_a=[(e, layer, k) for e in layers], along_b=[(d, 2)] if s == d else [])

    def from_a(j, d, s, k):
        layer = d if s == 2 else s
        step = 1 - 2 * d
        a_, b_ = turn(a - (2 if s == 2 else 1) * step), turn(b + off(k))
        arrived(block(j, layer, a_, b_), ring_sem.at[d, s, k, j])
        pass_on(j, layer, a_, b_, along_a=[(d, 2, k)] if s == d else [])

    for j in kinds:
        from_b(j, 0, 0)
        from_b(j, 1, 1)
        from_a(j, 0, 0, 3)
        from_a(j, 1, 1, 3)
    for j in kinds:
        from_b(j, 0, 1)
        from_b(j, 1, 0)
    for j in kinds:
        from_b(j, 0, 2)
        from_b(j, 1, 2)
    for k in range(3):
        for j in kinds:
            from_a(j, 0, 0, (1, 2, 0)[k])
            from_a(j, 1, 1, (2, 1, 0)[k])
    for k in (3, 1, 2, 0):
        for j in kinds:
            from_a(j, 0, 1, k)
            from_a(j, 1, 0, k)
    for k in (3, 1, 2, 0):
        for j in kinds:
            from_a(j, 0, 2, k)
            from_a(j, 1, 2, k)

    for j in kinds:
        arrived(o[j].at[:, :, :, 0], back_sem.at[j])
        arrived(o[j].at[:, :, :, 0], mate_out.at[j])
        arrived(ring[j], ring_out.at[j])
        arrived(pair[j], pair_out.at[j])
    arrived(parts.at[pl.ds(0, n - 1)], part_out)


def write_out(*refs):
    sem = refs[-1]
    moves = [pltpu.make_async_copy(src, dst, sem.at[i]) for i, (src, dst) in enumerate(zip(refs[:9], refs[9:18], strict=True))]
    for one in moves:
        one.start()
    for one in moves:
        one.wait()


def solution(mesh):
    n = mesh.shape["dp"]
    side = math.isqrt(n // CORES)

    def step(*arrays):
        terms, weights, ms, vs = (arrays[i : i + 3] for i in (0, 3, 6, 9))
        blocks = [(one.shape[0], side, side, CORES, *one.shape[1:]) for one in ms]
        terms = [one.reshape(s) for one, s in zip(terms, blocks, strict=True)]
        whole = [one.reshape(s) for one, s in zip(weights, blocks, strict=True)]
        f32, bf16 = jnp.float32, jnp.bfloat16
        dma = pltpu.SemaphoreType.DMA
        tail = [s[-2:] for s in blocks]
        out = pl.pallas_call(
            functools.partial(kernel, n, side),
            out_shape=[pltpu.VMEM(s, bf16) for s in blocks] + [pltpu.VMEM(one.shape, f32) for one in (*ms, *vs)],
            in_specs=[pl.BlockSpec(memory_space=pltpu.HBM)] * 12,
            out_specs=[pl.BlockSpec(memory_space=pltpu.VMEM)] * 9,
            scratch_shapes=[
                *(pltpu.VMEM((2, 3, side, *s), bf16) for s in tail),
                *(pltpu.VMEM((2, 3, *s), bf16) for s in tail),
                *(pltpu.VMEM(one.shape, f32) for one in ms),
                *(pltpu.VMEM(one.shape, bf16) for one in ms),
                *(pltpu.VMEM(one.shape, bf16) for one in ms),
                pltpu.VMEM((n, 1, 128), f32),
                dma((2, 4, side, 3)),
                dma((2, 4, side, 3)),
                dma((2, 3, side, 3)),
                dma((2, 3, 3)),
                dma(()),
                dma((3, 3)),
                dma((3,)),
                dma((3,)),
                dma((3,)),
                dma((3,)),
                dma(()),
            ],
            compiler_params=pltpu.CompilerParams(collective_id=0, has_side_effects=True, vmem_limit_bytes=24 << 20),
        )(*(pltpu.with_memory_space_constraint(one, pltpu.HBM) for one in (*terms, *whole, *ms, *vs)))
        out = pl.pallas_call(
            write_out,
            out_shape=[jax.ShapeDtypeStruct(one.shape, one.dtype) for one in out],
            in_specs=[pl.BlockSpec(memory_space=pltpu.VMEM)] * 9,
            out_specs=[pl.BlockSpec(memory_space=pltpu.HBM)] * 9,
            scratch_shapes=[dma((9,))],
            compiler_params=pltpu.CompilerParams(vmem_limit_bytes=1 << 20),
        )(*out)
        return (*(one.reshape(w.shape) for one, w in zip(out[:3], weights, strict=True)), *out[3:])

    all_of, cut = P(None, None, None), P(None, "dp", None)
    return jax.shard_map(
        step,
        mesh=mesh,
        in_specs=(P(("rep", "dp"), None, None, None),) * 3 + (all_of,) * 3 + (cut,) * 6,
        out_specs=(P("rep", None, None),) * 3 + (P("rep", "dp", None),) * 6,
        check_vma=False,
    )
```

```python
import functools
import math

import jax
import jax.numpy as jnp
from jax import lax
from jax.experimental import pallas as pl
from jax.experimental.pallas import tpu as pltpu
from jax.sharding import PartitionSpec as P

CORES = 2
ROWS, COLS = 16, 512


def strips(shape):
    rows, cols = shape
    if rows > ROWS:
        return rows // ROWS, lambda i: (pl.ds(pl.multiple_of(i * ROWS, ROWS), ROWS), slice(None))
    return cols // COLS, lambda i: (slice(None), pl.ds(pl.multiple_of(i * COLS, COLS), COLS))


def kernel(n, side, *refs):
    (t, w, m, v, o, mo, vo, ring, pair, kept, g, held) = (refs[3 * i : 3 * i + 3] for i in range(12))
    (
        parts, own_sem, first_sem, mate_sem, ring_sem, pair_sem, part_sem, state_sem, back_sem,
        mate_out, ring_out, pair_out, part_out,
    ) = refs[36:]
    kinds, layers = range(3), range(2)
    f32, bf16 = jnp.float32, jnp.bfloat16

    me = lax.axis_index("dp")
    core, chip = lax.rem(me, CORES), lax.div(me, CORES)
    x, y = lax.div(chip, side), lax.rem(chip, side)
    a, b = x + core * (y - x), y + core * (x - y)
    mate = {"dp": me + 1 - 2 * core}

    def turn(i):
        return lax.rem(i + side, side)

    def place(a_, b_, core_=core):
        return a_ + core_ * (b_ - a_), b_ + core_ * (a_ - b_)

    def device(a_, b_):
        x_, y_ = place(a_, b_)
        return {"dp": (x_ * side + y_) * CORES + core}

    near_a = [device(turn(a + 1), b), device(turn(a - 1), b)]
    near_b = [device(a, turn(b + 1)), device(a, turn(b - 1))]

    def off(k):
        return 2 + k - 3 * (k // 2) - 2 * (k // 3)

    def role(d, s, k, a_, b_):
        step = 1 - 2 * d
        to = turn(a_ + (0 if s == 3 else step + step * (s == 0)))
        return (1 - d if s == 1 else d), to, turn(b_ + off(k))

    def block(j, layer, a_, b_):
        return o[j].at[(layer, *place(a_, b_), core)]

    def other(j, layer, a_, b_):
        return o[j].at[(layer, *place(a_, b_), 1 - core)]

    def load(s, k):
        for d in layers:
            layer, a_, b_ = role(d, s, k, a, b)
            for j in kinds:
                pltpu.make_async_copy(t[j].at[(layer, *place(a_, b_), core)], block(j, layer, a_, b_), own_sem.at[s]).start()

    def for_mate(s, k):
        for d in layers:
            layer, a_, b_ = role(d, s, k, b, a)
            at = place(a_, b_, 1 - core)
            for j in kinds:
                yield d, j, t[j].at[(layer, *at, 1 - core)], o[j].at[(layer, *at, core)]

    def hand(s, k):
        for _, j, src, dst in for_mate(s, k):
            pltpu.make_async_remote_copy(src, dst, mate_out.at[j], mate_sem.at[s, k], device_id=mate).start()

    def arrived(ref, sem):
        pltpu.make_async_copy(ref, ref, sem).wait()

    def send(src, dst, out_sem, sem, to):
        pltpu.make_async_remote_copy(src, dst, out_sem, sem, device_id=to).start()

    def total(j, d, s, k, more=(), into=None):
        layer, a_, b_ = role(d, s, k, a, b)
        mine, its = block(j, layer, a_, b_), other(j, layer, a_, b_)
        into = mine if into is None else into
        count, cut = strips(mine.shape)

        @pl.loop(0, count)
        def _(i):
            at = cut(i)
            so_far = mine[at].astype(f32) + its[at].astype(f32)
            for one in more:
                so_far += one[at].astype(f32)
            into[at] = so_far.astype(into.dtype)

        return mine

    barrier = pltpu.get_barrier_semaphore()
    for to in (mate, *near_a, *near_b):
        pl.semaphore_signal(barrier, inc=1, device_id=to)
    for d, j, src, _ in for_mate(0, 0):
        pltpu.make_async_copy(src, g[j].at[d], state_sem.at[0]).start()
    pl.loop(0, side)(functools.partial(load, 0))
    pl.semaphore_wait(barrier, 5)

    arrived(pair[0], state_sem.at[0])
    for d, j, _, dst in for_mate(0, 0):
        send(g[j].at[d], dst, mate_out.at[j], first_sem.at[d, j], mate)
    pl.loop(1, side)(functools.partial(hand, 0))
    for s in (1, 2, 3):
        pl.loop(0, side)(functools.partial(load, s))
    for j in kinds:
        x_, y_ = place(a, b)
        pltpu.make_async_copy(w[j].at[:, x_, y_, core], held[j], state_sem.at[0]).start()
        pltpu.make_async_copy(m[j], mo[j], state_sem.at[1]).start()
        pltpu.make_async_copy(v[j], vo[j], state_sem.at[2]).start()

    def out_along_a(s, k, first=False):
        if not first:
            arrived(pair[0], mate_sem.at[s, k])
        for j in kinds:
            for d in layers:
                more = ()
                if first:
                    arrived(g[j].at[d], first_sem.at[d, j])
                if s == 2:
                    arrived(ring[j].at[d, 0, k], ring_sem.at[d, 0, k, j])
                    more = (ring[j].at[d, 0, k],)
                mine = total(j, d, s, k, more)
                send(mine, ring[j].at[d, s, k], ring_out.at[j], ring_sem.at[d, s, k, j], near_a[d])
        hand(s + 1, k)

    arrived(ring[0], own_sem.at[0])
    out_along_a(0, 0, True)
    pl.loop(1, side)(functools.partial(out_along_a, 0))
    for s in (1, 2):
        arrived(ring[0], own_sem.at[s])
        pl.loop(0, side)(functools.partial(out_along_a, s))

    def last(j, layer, k, more=(), into=None):
        came = [ring[j].at[layer, 2, k], ring[j].at[1 - layer, 1, k]]
        arrived(came[0], ring_sem.at[layer, 2, k, j])
        arrived(came[1], ring_sem.at[1 - layer, 1, k, j])
        return total(j, layer, 3, k, (*came, *more), into)

    arrived(ring[0], own_sem.at[3])
    for k in range(side):
        arrived(pair[0], mate_sem.at[3, k])

    def onward(j, layer, k, d, s, more=()):
        send(last(j, layer, k, more), pair[j].at[d, s], pair_out.at[j], pair_sem.at[d, s, j], near_b[d])

    for j in kinds:
        for d in layers:
            onward(j, d, 0, d, 0)
    for j in kinds:
        onward(j, 0, 1, 1, 1)
        onward(j, 1, 2, 0, 1)
    for j in kinds:
        for layer, k, d in ((1, 1, 1), (0, 2, 0)):
            arrived(pair[j].at[d, 0], pair_sem.at[d, 0, j])
            onward(j, layer, k, d, 2, (pair[j].at[d, 0],))
    for j in kinds:
        for layer in layers:
            last(j, layer, 3, into=kept[j].at[layer])

    for j in kinds:
        arrived(o[j].at[:, :, :, 0], mate_out.at[j])
    squares = jnp.zeros((ROWS, COLS), f32)
    for j in kinds:
        for layer in layers:
            came = [pair[j].at[layer, 2], pair[j].at[1 - layer, 1]]
            arrived(came[0], pair_sem.at[layer, 2, j])
            arrived(came[1], pair_sem.at[1 - layer, 1, j])
            count, cut = strips(came[0].shape)

            def finish(i, so_far, j=j, layer=layer, came=came, cut=cut):
                at = cut(i)
                grad = kept[j].at[layer][at] + came[0][at].astype(f32) + came[1][at].astype(f32)
                grad = grad.astype(bf16)
                g[j].at[layer][at] = grad
                grad = grad.astype(f32)
                return so_far + grad * grad

            squares = lax.fori_loop(0, count, finish, squares)
    by_lane = jnp.sum(squares, axis=0, keepdims=True)
    parts[me] = sum(by_lane[:, i * 128 : (i + 1) * 128] for i in range(COLS // 128))
    for j in kinds:
        arrived(ring[j], ring_out.at[j])
        arrived(pair[j], pair_out.at[j])

    far = CORES * (side + 1) * (side // 2)

    @pl.loop(0, n - 1)
    def _(i):
        ahead = lax.rem(far - 1 + i, n - 1) + 1
        send(parts.at[me], parts.at[me], part_out, part_sem, {"dp": lax.rem(me + ahead, n)})

    arrived(pair[0], state_sem.at[0])
    arrived(ring[0].at[0], state_sem.at[1])
    arrived(ring[0].at[0], state_sem.at[2])
    arrived(parts.at[pl.ds(0, n - 1)], part_sem)
    count = n * sum(math.prod(one.shape) for one in mo)
    whole = jnp.sum(jnp.sum(parts[...], axis=0), axis=1, keepdims=True)
    factor = jnp.minimum(1.0, 0.5 * lax.rsqrt(whole / count + 1e-30))

    def pass_on(j, layer, a_, b_, *, along_a=(), along_b=()):
        one = block(j, layer, a_, b_)
        for d, s in along_b:
            send(one, one, pair_out.at[j], pair_sem.at[d, s, j], near_b[d])
        for d, s, k in along_a:
            send(one, one, ring_out.at[j], ring_sem.at[d, s, k, j], near_a[d])
        send(one, one, mate_out.at[j], back_sem.at[j], mate)

    for layer in layers:
        for j in kinds:
            new = block(j, layer, a, b)
            count, cut = strips(new.shape)

            @pl.loop(0, count)
            def _(i, j=j, layer=layer, new=new, cut=cut):
                at = cut(i)
                grad = g[j].at[layer][at].astype(f32) * factor
                m_ = 0.9 * mo[j].at[layer][at] + 0.1 * grad
                v_ = 0.95 * vo[j].at[layer][at] + 0.05 * grad * grad
                w_ = held[j].at[layer][at].astype(f32)
                mo[j].at[layer][at] = m_
                vo[j].at[layer][at] = v_
                new[at] = (w_ - 0.02 * (m_ * lax.rsqrt(v_ + 1e-8) + 0.1 * w_)).astype(bf16)

            pass_on(j, layer, a, b, along_a=[(d, layer, 3) for d in layers], along_b=[(d, layer) for d in layers])

    def from_b(j, d, s):
        layer = d if s == 2 else s
        step = 1 - 2 * d
        b_ = turn(b - (2 if s == 2 else 1) * step)
        k = 0 if s == 2 else 1 + d
        arrived(block(j, layer, a, b_), pair_sem.at[d, s, j])
        pass_on(j, layer, a, b_, along_a=[(e, layer, k) for e in layers], along_b=[(d, 2)] if s == d else [])

    def from_a(j, d, s, k):
        layer = d if s == 2 else s
        step = 1 - 2 * d
        a_, b_ = turn(a - (2 if s == 2 else 1) * step), turn(b + off(k))
        arrived(block(j, layer, a_, b_), ring_sem.at[d, s, k, j])
        pass_on(j, layer, a_, b_, along_a=[(d, 2, k)] if s == d else [])

    for j in kinds:
        from_b(j, 0, 0)
        from_b(j, 1, 1)
        from_a(j, 0, 0, 3)
        from_a(j, 1, 1, 3)
    for j in kinds:
        from_b(j, 0, 1)
        from_b(j, 1, 0)
    for j in kinds:
        from_b(j, 0, 2)
        from_b(j, 1, 2)
    for k in range(3):
        for j in kinds:
            from_a(j, 0, 0, (1, 2, 0)[k])
            from_a(j, 1, 1, (2, 1, 0)[k])
    for k in (3, 1, 2, 0):
        for j in kinds:
            from_a(j, 0, 1, k)
            from_a(j, 1, 0, k)
    for k in (3, 1, 2, 0):
        for j in kinds:
            from_a(j, 0, 2, k)
            from_a(j, 1, 2, k)

    for j in kinds:
        arrived(o[j].at[:, :, :, 0], back_sem.at[j])
        arrived(o[j].at[:, :, :, 0], mate_out.at[j])
        arrived(ring[j], ring_out.at[j])
        arrived(pair[j], pair_out.at[j])
    arrived(parts.at[pl.ds(0, n - 1)], part_out)


def write_out(*refs):
    sem = refs[-1]
    moves = [pltpu.make_async_copy(src, dst, sem.at[i]) for i, (src, dst) in enumerate(zip(refs[:9], refs[9:18], strict=True))]
    for one in moves:
        one.start()
    for one in moves:
        one.wait()


def solution(mesh):
    n = mesh.shape["dp"]
    side = math.isqrt(n // CORES)

    def step(*arrays):
        terms, weights, ms, vs = (arrays[i : i + 3] for i in (0, 3, 6, 9))
        blocks = [(one.shape[0], side, side, CORES, *one.shape[1:]) for one in ms]
        terms = [one.reshape(s) for one, s in zip(terms, blocks, strict=True)]
        whole = [one.reshape(s) for one, s in zip(weights, blocks, strict=True)]
        f32, bf16 = jnp.float32, jnp.bfloat16
        dma = pltpu.SemaphoreType.DMA
        tail = [s[-2:] for s in blocks]
        out = pl.pallas_call(
            functools.partial(kernel, n, side),
            out_shape=[pltpu.VMEM(s, bf16) for s in blocks] + [pltpu.VMEM(one.shape, f32) for one in (*ms, *vs)],
            in_specs=[pl.BlockSpec(memory_space=pltpu.HBM)] * 12,
            out_specs=[pl.BlockSpec(memory_space=pltpu.VMEM)] * 9,
            scratch_shapes=[
                *(pltpu.VMEM((2, 3, side, *s), bf16) for s in tail),
                *(pltpu.VMEM((2, 3, *s), bf16) for s in tail),
                *(pltpu.VMEM(one.shape, f32) for one in ms),
                *(pltpu.VMEM(one.shape, bf16) for one in ms),
                *(pltpu.VMEM(one.shape, bf16) for one in ms),
                pltpu.VMEM((n, 1, 128), f32),
                dma((4,)),
                dma((2, 3)),
                dma((4, side)),
                dma((2, 3, side, 3)),
                dma((2, 3, 3)),
                dma(()),
                dma((3,)),
                dma((3,)),
                dma((3,)),
                dma((3,)),
                dma((3,)),
                dma(()),
            ],
            compiler_params=pltpu.CompilerParams(collective_id=0, has_side_effects=True, vmem_limit_bytes=24 << 20),
        )(*(pltpu.with_memory_space_constraint(one, pltpu.HBM) for one in (*terms, *whole, *ms, *vs)))
        out = pl.pallas_call(
            write_out,
            out_shape=[jax.ShapeDtypeStruct(one.shape, one.dtype) for one in out],
            in_specs=[pl.BlockSpec(memory_space=pltpu.VMEM)] * 9,
            out_specs=[pl.BlockSpec(memory_space=pltpu.HBM)] * 9,
            scratch_shapes=[dma((9,))],
            compiler_params=pltpu.CompilerParams(vmem_limit_bytes=1 << 20),
        )(*out)
        return (*(one.reshape(w.shape) for one, w in zip(out[:3], weights, strict=True)), *out[3:])

    all_of, cut = P(None, None, None), P(None, "dp", None)
    return jax.shard_map(
        step,
        mesh=mesh,
        in_specs=(P(("rep", "dp"), None, None, None),) * 3 + (all_of,) * 3 + (cut,) * 6,
        out_specs=(P("rep", None, None),) * 3 + (P("rep", "dp", None),) * 6,
        check_vma=False,
    )
```

```python
import functools
import math

import jax
import jax.numpy as jnp
from jax import lax
from jax.experimental import pallas as pl
from jax.experimental.pallas import tpu as pltpu
from jax.sharding import PartitionSpec as P

CORES = 2
ROWS, COLS = 16, 512


def strips(shape):
    rows, cols = shape
    if rows > ROWS:
        return rows // ROWS, lambda i: (pl.ds(pl.multiple_of(i * ROWS, ROWS), ROWS), slice(None))
    return cols // COLS, lambda i: (slice(None), pl.ds(pl.multiple_of(i * COLS, COLS), COLS))


def kernel(n, side, *refs):
    (t, w, m, v, o, mo, vo, ring, pair, kept, g, held) = (refs[3 * i : 3 * i + 3] for i in range(12))
    (
        parts, own_sem, first_sem, mate_sem, ring_sem, late_sem, pair_sem, part_sem, state_sem, back_sem,
        mate_out, ring_out, pair_out, part_out,
    ) = refs[36:]
    kinds, layers = range(3), range(2)
    f32, bf16 = jnp.float32, jnp.bfloat16

    me = lax.axis_index("dp")
    core, chip = lax.rem(me, CORES), lax.div(me, CORES)
    x, y = lax.div(chip, side), lax.rem(chip, side)
    a, b = x + core * (y - x), y + core * (x - y)
    mate = {"dp": me + 1 - 2 * core}

    def turn(i):
        return lax.rem(i + side, side)

    def place(a_, b_, core_=core):
        return a_ + core_ * (b_ - a_), b_ + core_ * (a_ - b_)

    def device(a_, b_):
        x_, y_ = place(a_, b_)
        return {"dp": (x_ * side + y_) * CORES + core}

    near_a = [device(turn(a + 1), b), device(turn(a - 1), b)]
    near_b = [device(a, turn(b + 1)), device(a, turn(b - 1))]

    def off(k):
        return 2 + k - 3 * (k // 2) - 2 * (k // 3)

    def role(d, s, k, a_, b_):
        step = 1 - 2 * d
        to = turn(a_ + (0 if s == 3 else step + step * (s == 0)))
        return (1 - d if s == 1 else d), to, turn(b_ + off(k))

    def block(j, layer, a_, b_):
        return o[j].at[(layer, *place(a_, b_), core)]

    def other(j, layer, a_, b_):
        return o[j].at[(layer, *place(a_, b_), 1 - core)]

    def load(s, k):
        for d in layers:
            layer, a_, b_ = role(d, s, k, a, b)
            for j in kinds:
                pltpu.make_async_copy(t[j].at[(layer, *place(a_, b_), core)], block(j, layer, a_, b_), own_sem.at[s]).start()

    def for_mate(s, k):
        for d in layers:
            layer, a_, b_ = role(d, s, k, b, a)
            at = place(a_, b_, 1 - core)
            for j in kinds:
                yield d, j, t[j].at[(layer, *at, 1 - core)], o[j].at[(layer, *at, core)]

    def hand(s, k):
        for _, j, src, dst in for_mate(s, k):
            pltpu.make_async_remote_copy(src, dst, mate_out.at[j], mate_sem.at[3 + k if s == 0 else s - 1], device_id=mate).start()

    def arrived(ref, sem):
        pltpu.make_async_copy(ref, ref, sem).wait()

    def along_a(j, d, s, k):
        return late_sem.at[d, k, j] if s == 2 else ring_sem.at[d, s, k]

    def arrived_a(ref, j, d, s, k):
        if s == 2:
            arrived(ref, late_sem.at[d, k, j])
        elif j == 0:
            arrived(pair[0].at[0], ring_sem.at[d, s, k])

    def send(src, dst, out_sem, sem, to):
        pltpu.make_async_remote_copy(src, dst, out_sem, sem, device_id=to).start()

    def total(j, d, s, k, more=(), into=None):
        layer, a_, b_ = role(d, s, k, a, b)
        mine, its = block(j, layer, a_, b_), other(j, layer, a_, b_)
        into = mine if into is None else into
        count, cut = strips(mine.shape)

        @pl.loop(0, count, unroll=4)
        def _(i):
            at = cut(i)
            so_far = mine[at].astype(f32) + its[at].astype(f32)
            for one in more:
                so_far += one[at].astype(f32)
            into[at] = so_far.astype(into.dtype)

        return mine

    barrier = pltpu.get_barrier_semaphore()
    for to in (mate, *near_a, *near_b):
        pl.semaphore_signal(barrier, inc=1, device_id=to)
    for d, j, src, _ in for_mate(0, 0):
        pltpu.make_async_copy(src, g[j].at[d], state_sem.at[0]).start()
    pl.loop(0, side)(functools.partial(load, 0))
    pl.semaphore_wait(barrier, 5)

    arrived(pair[0], state_sem.at[0])
    for d, j, _, dst in for_mate(0, 0):
        send(g[j].at[d], dst, mate_out.at[j], first_sem.at[d, j], mate)
    pl.loop(1, side)(functools.partial(hand, 0))

    def out_along_a(s, k, first=False):
        if s == 0 and not first:
            arrived(pair[0], mate_sem.at[3 + k])
        for j in kinds:
            for d in layers:
                more = ()
                if first:
                    arrived(g[j].at[d], first_sem.at[d, j])
                if s == 2:
                    arrived_a(ring[j].at[d, 0, k], j, d, 0, k)
                    more = (ring[j].at[d, 0, k],)
                mine = total(j, d, s, k, more)
                send(mine, ring[j].at[d, s, k], ring_out.at[j], along_a(j, d, s, k), near_a[d])
        hand(s + 1, k)

    arrived(ring[0], own_sem.at[0])
    out_along_a(0, 0, True)
    for s in (1, 2, 3):
        pl.loop(0, side)(functools.partial(load, s))
    for j in kinds:
        x_, y_ = place(a, b)
        pltpu.make_async_copy(w[j].at[:, x_, y_, core], held[j], state_sem.at[0]).start()
        pltpu.make_async_copy(m[j], mo[j], state_sem.at[1]).start()
        pltpu.make_async_copy(v[j], vo[j], state_sem.at[2]).start()
    pl.loop(1, side)(functools.partial(out_along_a, 0))
    for s in (1, 2):
        arrived(ring[0], own_sem.at[s])
        arrived(ring[0], mate_sem.at[s - 1])
        pl.loop(0, side)(functools.partial(out_along_a, s))

    def last(j, layer, k, more=(), into=None):
        came = [ring[j].at[layer, 2, k], ring[j].at[1 - layer, 1, k]]
        arrived_a(came[0], j, layer, 2, k)
        arrived_a(came[1], j, 1 - layer, 1, k)
        return total(j, layer, 3, k, (*came, *more), into)

    arrived(ring[0], own_sem.at[3])
    arrived(ring[0], mate_sem.at[2])

    def onward(j, layer, k, d, s, more=()):
        send(last(j, layer, k, more), pair[j].at[d, s], pair_out.at[j], pair_sem.at[d, s, j], near_b[d])

    for j in kinds:
        for d in layers:
            onward(j, d, 0, d, 0)
    for j in kinds:
        onward(j, 0, 1, 1, 1)
        onward(j, 1, 2, 0, 1)
    for j in kinds:
        for layer, k, d in ((1, 1, 1), (0, 2, 0)):
            arrived(pair[j].at[d, 0], pair_sem.at[d, 0, j])
            onward(j, layer, k, d, 2, (pair[j].at[d, 0],))
    for j in kinds:
        for layer in layers:
            last(j, layer, 3, into=kept[j].at[layer])

    for j in kinds:
        arrived(o[j].at[:, :, :, 0], mate_out.at[j])
    squares = jnp.zeros((ROWS, COLS), f32)
    for j in kinds:
        for layer in layers:
            came = [pair[j].at[layer, 2], pair[j].at[1 - layer, 1]]
            arrived(came[0], pair_sem.at[layer, 2, j])
            arrived(came[1], pair_sem.at[1 - layer, 1, j])
            count, cut = strips(came[0].shape)

            def finish(i, so_far, j=j, layer=layer, came=came, cut=cut):
                at = cut(i)
                grad = kept[j].at[layer][at] + came[0][at].astype(f32) + came[1][at].astype(f32)
                grad = grad.astype(bf16)
                g[j].at[layer][at] = grad
                grad = grad.astype(f32)
                return so_far + grad * grad

            squares = lax.fori_loop(0, count, finish, squares, unroll=4)
    by_lane = jnp.sum(squares, axis=0, keepdims=True)
    parts[me] = sum(by_lane[:, i * 128 : (i + 1) * 128] for i in range(COLS // 128))
    for j in kinds:
        arrived(ring[j], ring_out.at[j])
        arrived(pair[j], pair_out.at[j])

    @pl.loop(1, n)
    def _(i):
        send(parts.at[me], parts.at[me], part_out, part_sem, {"dp": lax.rem(me + i, n)})

    arrived(pair[0], state_sem.at[0])
    arrived(ring[0].at[0], state_sem.at[1])
    arrived(ring[0].at[0], state_sem.at[2])
    arrived(parts.at[pl.ds(0, n - 1)], part_sem)
    count = n * sum(math.prod(one.shape) for one in mo)
    whole = jnp.sum(jnp.sum(parts[...], axis=0), axis=1, keepdims=True)
    factor = jnp.minimum(1.0, 0.5 * lax.rsqrt(whole / count + 1e-30))

    def pass_on(j, layer, a_, b_, *, on_a=(), on_b=()):
        one = block(j, layer, a_, b_)
        for d, s in on_b:
            send(one, one, pair_out.at[j], pair_sem.at[d, s, j], near_b[d])
        for d, s, k in on_a:
            send(one, one, ring_out.at[j], along_a(j, d, s, k), near_a[d])
        send(one, one, mate_out.at[j], back_sem.at[j], mate)

    for layer in layers:
        for j in kinds:
            new = block(j, layer, a, b)
            count, cut = strips(new.shape)

            @pl.loop(0, count, unroll=4)
            def _(i, j=j, layer=layer, new=new, cut=cut):
                at = cut(i)
                grad = g[j].at[layer][at].astype(f32) * factor
                m_ = 0.9 * mo[j].at[layer][at] + 0.1 * grad
                v_ = 0.95 * vo[j].at[layer][at] + 0.05 * grad * grad
                w_ = held[j].at[layer][at].astype(f32)
                mo[j].at[layer][at] = m_
                vo[j].at[layer][at] = v_
                new[at] = (w_ - 0.02 * (m_ * lax.rsqrt(v_ + 1e-8) + 0.1 * w_)).astype(bf16)

            pass_on(j, layer, a, b, on_a=[(d, layer, 3) for d in layers], on_b=[(d, layer) for d in layers])

    def from_b(j, d, s):
        layer = d if s == 2 else s
        step = 1 - 2 * d
        b_ = turn(b - (2 if s == 2 else 1) * step)
        k = 0 if s == 2 else 1 + d
        arrived(block(j, layer, a, b_), pair_sem.at[d, s, j])
        pass_on(j, layer, a, b_, on_a=[(e, layer, k) for e in layers], on_b=[(d, 2)] if s == d else [])

    def from_a(j, d, s, k):
        layer = d if s == 2 else s
        step = 1 - 2 * d
        a_, b_ = turn(a - (2 if s == 2 else 1) * step), turn(b + off(k))
        arrived_a(block(j, layer, a_, b_), j, d, s, k)
        pass_on(j, layer, a_, b_, on_a=[(d, 2, k)] if s == d else [])

    for j in kinds:
        from_b(j, 0, 0)
        from_b(j, 1, 1)
        from_a(j, 0, 0, 3)
        from_a(j, 1, 1, 3)
    for j in kinds:
        from_b(j, 0, 1)
        from_b(j, 1, 0)
    for j in kinds:
        from_b(j, 0, 2)
        from_b(j, 1, 2)
    for k in range(3):
        for j in kinds:
            from_a(j, 0, 0, (1, 2, 0)[k])
            from_a(j, 1, 1, (2, 1, 0)[k])
    for k in (3, 1, 2, 0):
        for j in kinds:
            from_a(j, 0, 1, k)
            from_a(j, 1, 0, k)
    for k in (3, 1, 2, 0):
        for j in kinds:
            from_a(j, 0, 2, k)
            from_a(j, 1, 2, k)

    for j in kinds:
        arrived(o[j].at[:, :, :, 0], back_sem.at[j])
        arrived(o[j].at[:, :, :, 0], mate_out.at[j])
        arrived(ring[j], ring_out.at[j])
        arrived(pair[j], pair_out.at[j])
    arrived(parts.at[pl.ds(0, n - 1)], part_out)


def write_out(*refs):
    sem = refs[-1]
    moves = [pltpu.make_async_copy(src, dst, sem.at[i]) for i, (src, dst) in enumerate(zip(refs[:9], refs[9:18], strict=True))]
    for one in moves:
        one.start()
    for one in moves:
        one.wait()


def solution(mesh):
    n = mesh.shape["dp"]
    side = math.isqrt(n // CORES)

    def step(*arrays):
        terms, weights, ms, vs = (arrays[i : i + 3] for i in (0, 3, 6, 9))
        blocks = [(one.shape[0], side, side, CORES, *one.shape[1:]) for one in ms]
        terms = [one.reshape(s) for one, s in zip(terms, blocks, strict=True)]
        whole = [one.reshape(s) for one, s in zip(weights, blocks, strict=True)]
        f32, bf16 = jnp.float32, jnp.bfloat16
        dma = pltpu.SemaphoreType.DMA
        tail = [s[-2:] for s in blocks]
        out = pl.pallas_call(
            functools.partial(kernel, n, side),
            out_shape=[pltpu.VMEM(s, bf16) for s in blocks] + [pltpu.VMEM(one.shape, f32) for one in (*ms, *vs)],
            in_specs=[pl.BlockSpec(memory_space=pltpu.HBM)] * 12,
            out_specs=[pl.BlockSpec(memory_space=pltpu.VMEM)] * 9,
            scratch_shapes=[
                *(pltpu.VMEM((2, 3, side, *s), bf16) for s in tail),
                *(pltpu.VMEM((2, 3, *s), bf16) for s in tail),
                *(pltpu.VMEM(one.shape, f32) for one in ms),
                *(pltpu.VMEM(one.shape, bf16) for one in ms),
                *(pltpu.VMEM(one.shape, bf16) for one in ms),
                pltpu.VMEM((n, 1, 128), f32),
                dma((4,)),
                dma((2, 3)),
                dma((3 + side,)),
                dma((2, 2, side)),
                dma((2, side, 3)),
                dma((2, 3, 3)),
                dma(()),
                dma((3,)),
                dma((3,)),
                dma((3,)),
                dma((3,)),
                dma((3,)),
                dma(()),
            ],
            compiler_params=pltpu.CompilerParams(collective_id=0, has_side_effects=True, vmem_limit_bytes=24 << 20),
        )(*(pltpu.with_memory_space_constraint(one, pltpu.HBM) for one in (*terms, *whole, *ms, *vs)))
        out = pl.pallas_call(
            write_out,
            out_shape=[jax.ShapeDtypeStruct(one.shape, one.dtype) for one in out],
            in_specs=[pl.BlockSpec(memory_space=pltpu.VMEM)] * 9,
            out_specs=[pl.BlockSpec(memory_space=pltpu.HBM)] * 9,
            scratch_shapes=[dma((9,))],
            compiler_params=pltpu.CompilerParams(vmem_limit_bytes=1 << 20),
        )(*out)
        return (*(one.reshape(w.shape) for one, w in zip(out[:3], weights, strict=True)), *out[3:])

    all_of, cut = P(None, None, None), P(None, "dp", None)
    return jax.shard_map(
        step,
        mesh=mesh,
        in_specs=(P(("rep", "dp"), None, None, None),) * 3 + (all_of,) * 3 + (cut,) * 6,
        out_specs=(P("rep", None, None),) * 3 + (P("rep", "dp", None),) * 6,
        check_vma=False,
    )
```

```python
import functools
import math

import jax
import jax.numpy as jnp
from jax import lax
from jax.experimental import pallas as pl
from jax.experimental.pallas import tpu as pltpu
from jax.sharding import PartitionSpec as P

CORES = 2
ROWS, COLS = 16, 512


def strips(shape):
    rows, cols = shape
    if rows > ROWS:
        return rows // ROWS, lambda i: (pl.ds(pl.multiple_of(i * ROWS, ROWS), ROWS), slice(None))
    return cols // COLS, lambda i: (slice(None), pl.ds(pl.multiple_of(i * COLS, COLS), COLS))


def kernel(n, side, *refs):
    (t, w, m, v, o, mo, vo, ring, pair, kept, g, held) = (refs[3 * i : 3 * i + 3] for i in range(12))
    (
        parts, own_sem, first_sem, mate_sem, ring_sem, late_sem, pair_sem, part_sem, state_sem, back_sem,
        mate_out, ring_out, pair_out, part_out,
    ) = refs[36:]
    kinds, layers = range(3), range(2)
    f32, bf16 = jnp.float32, jnp.bfloat16

    me = lax.axis_index("dp")
    core, chip = lax.rem(me, CORES), lax.div(me, CORES)
    x, y = lax.div(chip, side), lax.rem(chip, side)
    a, b = x + core * (y - x), y + core * (x - y)
    mate = {"dp": me + 1 - 2 * core}

    def turn(i):
        return lax.rem(i + 2 * side, side)

    def place(a_, b_, core_=core):
        return a_ + core_ * (b_ - a_), b_ + core_ * (a_ - b_)

    def device(a_, b_):
        x_, y_ = place(a_, b_)
        return {"dp": (x_ * side + y_) * CORES + core}

    near_a = [device(turn(a - 1), b), device(turn(a + 1), b)]
    near_b = [device(a, turn(b + 1)), device(a, turn(b - 1))]

    def off(k):
        return 2 + k - 3 * (k // 2) - 2 * (k // 3)

    def role(d, s, k, a_, b_):
        step = 2 * d - 1
        to = turn(a_ + (0 if s == 3 else step + step * (s == 0)))
        return (1 - d if s == 1 else d), to, turn(b_ + off(k))

    def block(j, layer, a_, b_):
        return o[j].at[(layer, *place(a_, b_), core)]

    def other(j, layer, a_, b_):
        return o[j].at[(layer, *place(a_, b_), 1 - core)]

    def load(s, k):
        for d in layers:
            layer, a_, b_ = role(d, s, k, a, b)
            for j in kinds:
                pltpu.make_async_copy(t[j].at[(layer, *place(a_, b_), core)], block(j, layer, a_, b_), own_sem.at[s]).start()

    def for_mate(s, k):
        at = [role(d, s, k, b, a) for d in layers]
        for j in kinds:
            for d in layers:
                layer, to = at[d][0], place(*at[d][1:], 1 - core)
                yield d, j, t[j].at[(layer, *to, 1 - core)], o[j].at[(layer, *to, core)]

    def hand(s, k):
        for _, j, src, dst in for_mate(s, k):
            pltpu.make_async_remote_copy(src, dst, mate_out.at[j], mate_sem.at[3 + k if s == 0 else s - 1], device_id=mate).start()

    def arrived(ref, sem):
        pltpu.make_async_copy(ref, ref, sem).wait()

    def along_a(j, d, s, k):
        return late_sem.at[d, k, j] if s == 2 else ring_sem.at[d, s, k]

    def arrived_a(ref, j, d, s, k):
        if s == 2:
            arrived(ref, late_sem.at[d, k, j])
        elif j == 0:
            arrived(pair[0].at[0], ring_sem.at[d, s, k])

    def send(src, dst, out_sem, sem, to):
        pltpu.make_async_remote_copy(src, dst, out_sem, sem, device_id=to).start()

    def total(j, d, s, k, more=(), into=None):
        layer, a_, b_ = role(d, s, k, a, b)
        mine, its = block(j, layer, a_, b_), other(j, layer, a_, b_)
        into = mine if into is None else into
        count, cut = strips(mine.shape)

        @pl.loop(0, count, unroll=4)
        def _(i):
            at = cut(i)
            so_far = mine[at].astype(f32) + its[at].astype(f32)
            for one in more:
                so_far += one[at].astype(f32)
            into[at] = so_far.astype(into.dtype)

        return mine

    barrier = pltpu.get_barrier_semaphore()
    for to in (mate, *near_a, *near_b):
        pl.semaphore_signal(barrier, inc=1, device_id=to)
    pl.loop(0, side)(functools.partial(load, 0))
    pl.semaphore_wait(barrier, 5)

    for d, j, src, dst in for_mate(0, 0):
        send(src, dst, mate_out.at[j], first_sem.at[d, j], mate)
    pl.loop(1, side)(functools.partial(hand, 0))

    def out_along_a(s, k, first=False):
        if s == 0 and not first:
            arrived(pair[0], mate_sem.at[3 + k])
        for j in kinds:
            for d in layers:
                more = ()
                if first:
                    arrived(g[j].at[d], first_sem.at[d, j])
                if s == 2:
                    arrived_a(ring[j].at[d, 0, k], j, d, 0, k)
                    more = (ring[j].at[d, 0, k],)
                mine = total(j, d, s, k, more)
                send(mine, ring[j].at[d, s, k], ring_out.at[j], along_a(j, d, s, k), near_a[d])
        hand(s + 1, k)

    arrived(ring[0], own_sem.at[0])
    out_along_a(0, 0, True)
    for s in (1, 2, 3):
        pl.loop(0, side)(functools.partial(load, s))
    for j in kinds:
        x_, y_ = place(a, b)
        pltpu.make_async_copy(w[j].at[:, x_, y_, core], held[j], state_sem.at[0]).start()
        pltpu.make_async_copy(m[j], mo[j], state_sem.at[1]).start()
        pltpu.make_async_copy(v[j], vo[j], state_sem.at[2]).start()
    pl.loop(1, side)(functools.partial(out_along_a, 0))
    for s in (1, 2):
        arrived(ring[0], own_sem.at[s])
        arrived(ring[0], mate_sem.at[s - 1])
        pl.loop(0, side)(functools.partial(out_along_a, s))

    def last(j, layer, k, more=(), into=None):
        came = [ring[j].at[layer, 2, k], ring[j].at[1 - layer, 1, k]]
        arrived_a(came[0], j, layer, 2, k)
        arrived_a(came[1], j, 1 - layer, 1, k)
        return total(j, layer, 3, k, (*came, *more), into)

    arrived(ring[0], own_sem.at[3])
    arrived(ring[0], mate_sem.at[2])

    def onward(j, layer, k, d, s, more=()):
        send(last(j, layer, k, more), pair[j].at[d, s], pair_out.at[j], pair_sem.at[d, s, j], near_b[d])

    for j in kinds:
        for d in layers:
            onward(j, d, 0, d, 0)
    for j in kinds:
        onward(j, 0, 1, 1, 1)
        onward(j, 1, 2, 0, 1)
    for j in kinds:
        for layer, k, d in ((1, 1, 1), (0, 2, 0)):
            arrived(pair[j].at[d, 0], pair_sem.at[d, 0, j])
            onward(j, layer, k, d, 2, (pair[j].at[d, 0],))
    for j in kinds:
        for layer in layers:
            last(j, layer, 3, into=kept[j].at[layer])

    for j in kinds:
        arrived(o[j].at[:, :, :, 0], mate_out.at[j])
    squares = jnp.zeros((ROWS, COLS), f32)
    for j in kinds:
        for layer in layers:
            came = [pair[j].at[layer, 2], pair[j].at[1 - layer, 1]]
            arrived(came[0], pair_sem.at[layer, 2, j])
            arrived(came[1], pair_sem.at[1 - layer, 1, j])
            count, cut = strips(came[0].shape)

            def finish(i, so_far, j=j, layer=layer, came=came, cut=cut):
                at = cut(i)
                grad = kept[j].at[layer][at] + came[0][at].astype(f32) + came[1][at].astype(f32)
                grad = grad.astype(bf16)
                g[j].at[layer][at] = grad
                grad = grad.astype(f32)
                return so_far + grad * grad

            squares = lax.fori_loop(0, count, finish, squares, unroll=4)
    by_lane = jnp.sum(squares, axis=0, keepdims=True)
    parts[me] = sum(by_lane[:, i * 128 : (i + 1) * 128] for i in range(COLS // 128))
    for j in kinds:
        arrived(ring[j], ring_out.at[j])
        arrived(pair[j], pair_out.at[j])

    @pl.loop(1, n)
    def _(i):
        send(parts.at[me], parts.at[me], part_out, part_sem, {"dp": lax.rem(me + i, n)})

    arrived(pair[0], state_sem.at[0])
    arrived(ring[0].at[0], state_sem.at[1])
    arrived(ring[0].at[0], state_sem.at[2])
    arrived(parts.at[pl.ds(0, n - 1)], part_sem)
    count = n * sum(math.prod(one.shape) for one in mo)
    whole = jnp.sum(jnp.sum(parts[...], axis=0), axis=1, keepdims=True)
    factor = jnp.minimum(1.0, 0.5 * lax.rsqrt(whole / count + 1e-30))

    def pass_on(j, layer, a_, b_, *, on_a=(), on_b=()):
        one = block(j, layer, a_, b_)
        for d, s in on_b:
            send(one, one, pair_out.at[j], pair_sem.at[d, s, j], near_b[d])
        for d, s, k in on_a:
            send(one, one, ring_out.at[j], along_a(j, d, s, k), near_a[d])
        send(one, one, mate_out.at[j], back_sem.at[j], mate)

    for layer in layers:
        for j in kinds:
            new = block(j, layer, a, b)
            count, cut = strips(new.shape)

            @pl.loop(0, count, unroll=4)
            def _(i, j=j, layer=layer, new=new, cut=cut):
                at = cut(i)
                grad = g[j].at[layer][at].astype(f32) * factor
                m_ = 0.9 * mo[j].at[layer][at] + 0.1 * grad
                v_ = 0.95 * vo[j].at[layer][at] + 0.05 * grad * grad
                w_ = held[j].at[layer][at].astype(f32)
                mo[j].at[layer][at] = m_
                vo[j].at[layer][at] = v_
                new[at] = (w_ - 0.02 * (m_ * lax.rsqrt(v_ + 1e-8) + 0.1 * w_)).astype(bf16)

            pass_on(j, layer, a, b, on_a=[(d, layer, 3) for d in layers], on_b=[(d, layer) for d in layers])

    def from_b(j, d, s):
        layer = d if s == 2 else s
        step = 1 - 2 * d
        b_ = turn(b - (2 if s == 2 else 1) * step)
        k = 0 if s == 2 else 1 + d
        arrived(block(j, layer, a, b_), pair_sem.at[d, s, j])
        pass_on(j, layer, a, b_, on_a=[(e, layer, k) for e in layers], on_b=[(d, 2)] if s == d else [])

    def from_a(j, d, s, k):
        layer = d if s == 2 else s
        step = 2 * d - 1
        a_, b_ = turn(a - (2 if s == 2 else 1) * step), turn(b + off(k))
        arrived_a(block(j, layer, a_, b_), j, d, s, k)
        pass_on(j, layer, a_, b_, on_a=[(d, 2, k)] if s == d else [])

    for j in kinds:
        from_b(j, 0, 0)
        from_b(j, 1, 1)
        from_a(j, 0, 0, 3)
        from_a(j, 1, 1, 3)
    for j in kinds:
        from_b(j, 0, 1)
        from_b(j, 1, 0)
    for j in kinds:
        from_b(j, 0, 2)
        from_b(j, 1, 2)
    for k in range(3):
        for j in kinds:
            from_a(j, 0, 0, (1, 2, 0)[k])
            from_a(j, 1, 1, (2, 1, 0)[k])
    for k in (3, 1, 2, 0):
        for j in kinds:
            from_a(j, 0, 1, k)
            from_a(j, 1, 0, k)
    for k in (3, 1, 2, 0):
        for j in kinds:
            from_a(j, 0, 2, k)
            from_a(j, 1, 2, k)

    for j in kinds:
        arrived(o[j].at[:, :, :, 0], back_sem.at[j])
        arrived(o[j].at[:, :, :, 0], mate_out.at[j])
        arrived(ring[j], ring_out.at[j])
        arrived(pair[j], pair_out.at[j])
    arrived(parts.at[pl.ds(0, n - 1)], part_out)


def write_out(*refs):
    sem = refs[-1]
    moves = [pltpu.make_async_copy(src, dst, sem.at[i]) for i, (src, dst) in enumerate(zip(refs[:9], refs[9:18], strict=True))]
    for one in moves:
        one.start()
    for one in moves:
        one.wait()


def solution(mesh):
    n = mesh.shape["dp"]
    side = math.isqrt(n // CORES)

    def step(*arrays):
        terms, weights, ms, vs = (arrays[i : i + 3] for i in (0, 3, 6, 9))
        blocks = [(one.shape[0], side, side, CORES, *one.shape[1:]) for one in ms]
        terms = [one.reshape(s) for one, s in zip(terms, blocks, strict=True)]
        whole = [one.reshape(s) for one, s in zip(weights, blocks, strict=True)]
        f32, bf16 = jnp.float32, jnp.bfloat16
        dma = pltpu.SemaphoreType.DMA
        tail = [s[-2:] for s in blocks]
        out = pl.pallas_call(
            functools.partial(kernel, n, side),
            out_shape=[pltpu.VMEM(s, bf16) for s in blocks] + [pltpu.VMEM(one.shape, f32) for one in (*ms, *vs)],
            in_specs=[pl.BlockSpec(memory_space=pltpu.HBM)] * 12,
            out_specs=[pl.BlockSpec(memory_space=pltpu.VMEM)] * 9,
            scratch_shapes=[
                *(pltpu.VMEM((2, 3, side, *s), bf16) for s in tail),
                *(pltpu.VMEM((2, 3, *s), bf16) for s in tail),
                *(pltpu.VMEM(one.shape, f32) for one in ms),
                *(pltpu.VMEM(one.shape, bf16) for one in ms),
                *(pltpu.VMEM(one.shape, bf16) for one in ms),
                pltpu.VMEM((n, 1, 128), f32),
                dma((4,)),
                dma((2, 3)),
                dma((3 + side,)),
                dma((2, 2, side)),
                dma((2, side, 3)),
                dma((2, 3, 3)),
                dma(()),
                dma((3,)),
                dma((3,)),
                dma((3,)),
                dma((3,)),
                dma((3,)),
                dma(()),
            ],
            compiler_params=pltpu.CompilerParams(collective_id=0, has_side_effects=True, vmem_limit_bytes=24 << 20),
        )(*(pltpu.with_memory_space_constraint(one, pltpu.HBM) for one in (*terms, *whole, *ms, *vs)))
        out = pl.pallas_call(
            write_out,
            out_shape=[jax.ShapeDtypeStruct(one.shape, one.dtype) for one in out],
            in_specs=[pl.BlockSpec(memory_space=pltpu.VMEM)] * 9,
            out_specs=[pl.BlockSpec(memory_space=pltpu.HBM)] * 9,
            scratch_shapes=[dma((9,))],
            compiler_params=pltpu.CompilerParams(vmem_limit_bytes=1 << 20),
        )(*out)
        return (*(one.reshape(w.shape) for one, w in zip(out[:3], weights, strict=True)), *out[3:])

    all_of, cut = P(None, None, None), P(None, "dp", None)
    return jax.shard_map(
        step,
        mesh=mesh,
        in_specs=(P(("rep", "dp"), None, None, None),) * 3 + (all_of,) * 3 + (cut,) * 6,
        out_specs=(P("rep", None, None),) * 3 + (P("rep", "dp", None),) * 6,
        check_vma=False,
    )
```

```python
import functools
import math

import jax
import jax.numpy as jnp
from jax import lax
from jax.experimental import pallas as pl
from jax.experimental.pallas import tpu as pltpu
from jax.sharding import PartitionSpec as P

CORES = 2
ROWS, COLS = 16, 512


def strips(shape):
    rows, cols = shape
    if rows > ROWS:
        return rows // ROWS, lambda i: (pl.ds(pl.multiple_of(i * ROWS, ROWS), ROWS), slice(None))
    return cols // COLS, lambda i: (slice(None), pl.ds(pl.multiple_of(i * COLS, COLS), COLS))


def kernel(n, side, *refs):
    (t, w, m, v, o, mo, vo, ring, pair, kept, g, held) = (refs[3 * i : 3 * i + 3] for i in range(12))
    (
        parts, own_sem, first_sem, mate_sem, ring_sem, late_sem, pair_sem, part_sem, state_sem, back_sem,
        mate_out, ring_out, pair_out, part_out,
    ) = refs[36:]
    kinds, layers = range(3), range(2)
    f32, bf16 = jnp.float32, jnp.bfloat16

    me = lax.axis_index("dp")
    core, chip = lax.rem(me, CORES), lax.div(me, CORES)
    x, y = lax.div(chip, side), lax.rem(chip, side)
    a, b = x + core * (y - x), y + core * (x - y)
    mate = {"dp": me + 1 - 2 * core}

    def turn(i):
        return lax.rem(i + 2 * side, side)

    def place(a_, b_, core_=core):
        return a_ + core_ * (b_ - a_), b_ + core_ * (a_ - b_)

    def device(a_, b_):
        x_, y_ = place(a_, b_)
        return {"dp": (x_ * side + y_) * CORES + core}

    near_a = [device(turn(a - 1), b), device(turn(a + 1), b)]
    near_b = [device(a, turn(b + 1)), device(a, turn(b - 1))]

    def off(k):
        return 2 + k - 3 * (k // 2) - 2 * (k // 3)

    def role(d, s, k, a_, b_):
        step = 2 * d - 1
        to = turn(a_ + (0 if s == 3 else step + step * (s == 0)))
        return (1 - d if s == 1 else d), to, turn(b_ + off(k))

    def block(j, layer, a_, b_):
        return o[j].at[(layer, *place(a_, b_), core)]

    def other(j, layer, a_, b_):
        return o[j].at[(layer, *place(a_, b_), 1 - core)]

    def load(s, k):
        for d in layers:
            layer, a_, b_ = role(d, s, k, a, b)
            for j in kinds:
                pltpu.make_async_copy(t[j].at[(layer, *place(a_, b_), core)], block(j, layer, a_, b_), own_sem.at[s]).start()

    def for_mate(s, k):
        at = [role(d, s, k, b, a) for d in layers]
        for j in kinds:
            for d in layers:
                layer, to = at[d][0], place(*at[d][1:], 1 - core)
                yield d, j, t[j].at[(layer, *to, 1 - core)], o[j].at[(layer, *to, core)]

    def hand(s, k):
        for _, j, src, dst in for_mate(s, k):
            pltpu.make_async_remote_copy(src, dst, mate_out.at[j], mate_sem.at[3 + k if s == 0 else s - 1], device_id=mate).start()

    def arrived(ref, sem):
        pltpu.make_async_copy(ref, ref, sem).wait()

    def along_a(j, d, s, k):
        return late_sem.at[d, k, j] if s == 2 else ring_sem.at[d, s, k]

    def arrived_a(ref, j, d, s, k):
        if s == 2:
            arrived(ref, late_sem.at[d, k, j])
        elif j == 0:
            arrived(pair[0].at[0], ring_sem.at[d, s, k])

    def send(src, dst, out_sem, sem, to):
        pltpu.make_async_remote_copy(src, dst, out_sem, sem, device_id=to).start()

    def total(j, d, s, k, more=(), into=None):
        layer, a_, b_ = role(d, s, k, a, b)
        mine, its = block(j, layer, a_, b_), other(j, layer, a_, b_)
        into = mine if into is None else into
        count, cut = strips(mine.shape)

        @pl.loop(0, count, unroll=4)
        def _(i):
            at = cut(i)
            so_far = mine[at].astype(f32) + its[at].astype(f32)
            for one in more:
                so_far += one[at].astype(f32)
            into[at] = so_far.astype(into.dtype)

        return mine

    barrier = pltpu.get_barrier_semaphore()
    for to in (mate, *near_a, *near_b):
        pl.semaphore_signal(barrier, inc=1, device_id=to)
    pl.loop(0, side)(functools.partial(load, 0))
    pl.semaphore_wait(barrier, 5)

    for d, j, src, dst in for_mate(0, 0):
        send(src, dst, mate_out.at[j], first_sem.at[d, j], mate)
    pl.loop(1, side)(functools.partial(hand, 0))

    def out_along_a(s, k, first=False):
        if s == 0 and not first:
            arrived(pair[0], mate_sem.at[3 + k])
        for j in kinds:
            for d in layers:
                more = ()
                if first:
                    arrived(g[j].at[d], first_sem.at[d, j])
                if s == 2:
                    arrived_a(ring[j].at[d, 0, k], j, d, 0, k)
                    more = (ring[j].at[d, 0, k],)
                mine = total(j, d, s, k, more)
                send(mine, ring[j].at[d, s, k], ring_out.at[j], along_a(j, d, s, k), near_a[d])
        hand(s + 1, k)

    arrived(ring[0], own_sem.at[0])
    out_along_a(0, 0, True)
    for s in (1, 2, 3):
        pl.loop(0, side)(functools.partial(load, s))
    for j in kinds:
        x_, y_ = place(a, b)
        pltpu.make_async_copy(w[j].at[:, x_, y_, core], held[j], state_sem.at[0]).start()
        pltpu.make_async_copy(m[j], mo[j], state_sem.at[1]).start()
        pltpu.make_async_copy(v[j], vo[j], state_sem.at[2]).start()
    pl.loop(1, side)(functools.partial(out_along_a, 0))
    for s in (1, 2):
        arrived(ring[0], own_sem.at[s])
        arrived(ring[0], mate_sem.at[s - 1])
        pl.loop(0, side)(functools.partial(out_along_a, s))

    def last(j, layer, k, more=(), into=None):
        came = [ring[j].at[layer, 2, k], ring[j].at[1 - layer, 1, k]]
        arrived_a(came[0], j, layer, 2, k)
        arrived_a(came[1], j, 1 - layer, 1, k)
        return total(j, layer, 3, k, (*came, *more), into)

    arrived(ring[0], own_sem.at[3])
    arrived(ring[0], mate_sem.at[2])

    def onward(j, layer, k, d, s, more=()):
        send(last(j, layer, k, more), pair[j].at[d, s], pair_out.at[j], pair_sem.at[d, s, j], near_b[d])

    for j in kinds:
        for d in layers:
            onward(j, d, 0, d, 0)
    for j in kinds:
        onward(j, 0, 1, 1, 1)
        onward(j, 1, 2, 0, 1)
    for j in kinds:
        for layer, k, d in ((1, 1, 1), (0, 2, 0)):
            arrived(pair[j].at[d, 0], pair_sem.at[d, 0, j])
            onward(j, layer, k, d, 2, (pair[j].at[d, 0],))
    for j in kinds:
        for layer in layers:
            last(j, layer, 3, into=kept[j].at[layer])

    for j in kinds:
        arrived(o[j].at[:, :, :, 0], mate_out.at[j])
    squares = jnp.zeros((ROWS, COLS), f32)
    for j in kinds:
        for layer in layers:
            came = [pair[j].at[layer, 2], pair[j].at[1 - layer, 1]]
            arrived(came[0], pair_sem.at[layer, 2, j])
            arrived(came[1], pair_sem.at[1 - layer, 1, j])
            count, cut = strips(came[0].shape)

            def finish(i, so_far, j=j, layer=layer, came=came, cut=cut):
                at = cut(i)
                grad = kept[j].at[layer][at] + came[0][at].astype(f32) + came[1][at].astype(f32)
                grad = grad.astype(bf16)
                g[j].at[layer][at] = grad
                grad = grad.astype(f32)
                return so_far + grad * grad

            squares = lax.fori_loop(0, count, finish, squares, unroll=4)
    by_lane = jnp.sum(squares, axis=0, keepdims=True)
    parts[me] = sum(by_lane[:, i * 128 : (i + 1) * 128] for i in range(COLS // 128))
    for j in kinds:
        arrived(ring[j], ring_out.at[j])
        arrived(pair[j], pair_out.at[j])

    @pl.loop(1, n, unroll=True)
    def _(i):
        send(parts.at[me], parts.at[me], part_out, part_sem, {"dp": lax.rem(me + i, n)})

    arrived(pair[0], state_sem.at[0])
    arrived(ring[0].at[0], state_sem.at[1])
    arrived(ring[0].at[0], state_sem.at[2])
    arrived(parts.at[pl.ds(0, n - 1)], part_sem)
    count = n * sum(math.prod(one.shape) for one in mo)
    whole = jnp.sum(jnp.sum(parts[...], axis=0), axis=1, keepdims=True)
    factor = jnp.minimum(1.0, 0.5 * lax.rsqrt(whole / count + 1e-30))

    def pass_on(j, layer, a_, b_, *, on_a=(), on_b=()):
        one = block(j, layer, a_, b_)
        for d, s in on_b:
            send(one, one, pair_out.at[j], pair_sem.at[d, s, j], near_b[d])
        for d, s, k in on_a:
            send(one, one, ring_out.at[j], along_a(j, d, s, k), near_a[d])
        send(one, one, mate_out.at[j], back_sem.at[j], mate)

    for layer in layers:
        for j in kinds:
            new = block(j, layer, a, b)
            count, cut = strips(new.shape)

            @pl.loop(0, count, unroll=4)
            def _(i, j=j, layer=layer, new=new, cut=cut):
                at = cut(i)
                grad = g[j].at[layer][at].astype(f32) * factor
                m_ = 0.9 * mo[j].at[layer][at] + 0.1 * grad
                v_ = 0.95 * vo[j].at[layer][at] + 0.05 * grad * grad
                w_ = held[j].at[layer][at].astype(f32)
                mo[j].at[layer][at] = m_
                vo[j].at[layer][at] = v_
                new[at] = (w_ - 0.02 * (m_ * lax.rsqrt(v_ + 1e-8) + 0.1 * w_)).astype(bf16)

            pass_on(j, layer, a, b, on_a=[(d, layer, 3) for d in layers], on_b=[(d, layer) for d in layers])

    def from_b(j, d, s):
        layer = d if s == 2 else s
        step = 1 - 2 * d
        b_ = turn(b - (2 if s == 2 else 1) * step)
        k = 0 if s == 2 else 1 + d
        arrived(block(j, layer, a, b_), pair_sem.at[d, s, j])
        pass_on(j, layer, a, b_, on_a=[(e, layer, k) for e in layers], on_b=[(d, 2)] if s == d else [])

    def from_a(j, d, s, k):
        layer = d if s == 2 else s
        step = 2 * d - 1
        a_, b_ = turn(a - (2 if s == 2 else 1) * step), turn(b + off(k))
        arrived_a(block(j, layer, a_, b_), j, d, s, k)
        pass_on(j, layer, a_, b_, on_a=[(d, 2, k)] if s == d else [])

    for j in kinds:
        from_b(j, 0, 0)
        from_b(j, 1, 1)
        from_a(j, 0, 0, 3)
        from_a(j, 1, 1, 3)
    for j in kinds:
        from_b(j, 0, 1)
        from_b(j, 1, 0)
    for j in kinds:
        from_b(j, 0, 2)
        from_b(j, 1, 2)
    for k in range(3):
        for j in kinds:
            from_a(j, 0, 0, (1, 2, 0)[k])
            from_a(j, 1, 1, (2, 1, 0)[k])
    for k in (3, 1, 2, 0):
        for j in kinds:
            from_a(j, 0, 1, k)
            from_a(j, 1, 0, k)
    for k in (3, 1, 2, 0):
        for j in kinds:
            from_a(j, 0, 2, k)
            from_a(j, 1, 2, k)

    for j in kinds:
        arrived(o[j].at[:, :, :, 0], back_sem.at[j])
        arrived(o[j].at[:, :, :, 0], mate_out.at[j])
        arrived(ring[j], ring_out.at[j])
        arrived(pair[j], pair_out.at[j])
    arrived(parts.at[pl.ds(0, n - 1)], part_out)


def write_out(*refs):
    sem = refs[-1]
    moves = [pltpu.make_async_copy(src, dst, sem.at[i]) for i, (src, dst) in enumerate(zip(refs[:9], refs[9:18], strict=True))]
    for one in moves:
        one.start()
    for one in moves:
        one.wait()


def solution(mesh):
    n = mesh.shape["dp"]
    side = math.isqrt(n // CORES)

    def step(*arrays):
        terms, weights, ms, vs = (arrays[i : i + 3] for i in (0, 3, 6, 9))
        blocks = [(one.shape[0], side, side, CORES, *one.shape[1:]) for one in ms]
        terms = [one.reshape(s) for one, s in zip(terms, blocks, strict=True)]
        whole = [one.reshape(s) for one, s in zip(weights, blocks, strict=True)]
        f32, bf16 = jnp.float32, jnp.bfloat16
        dma = pltpu.SemaphoreType.DMA
        tail = [s[-2:] for s in blocks]
        out = pl.pallas_call(
            functools.partial(kernel, n, side),
            out_shape=[pltpu.VMEM(s, bf16) for s in blocks] + [pltpu.VMEM(one.shape, f32) for one in (*ms, *vs)],
            in_specs=[pl.BlockSpec(memory_space=pltpu.HBM)] * 12,
            out_specs=[pl.BlockSpec(memory_space=pltpu.VMEM)] * 9,
            scratch_shapes=[
                *(pltpu.VMEM((2, 3, side, *s), bf16) for s in tail),
                *(pltpu.VMEM((2, 3, *s), bf16) for s in tail),
                *(pltpu.VMEM(one.shape, f32) for one in ms),
                *(pltpu.VMEM(one.shape, bf16) for one in ms),
                *(pltpu.VMEM(one.shape, bf16) for one in ms),
                pltpu.VMEM((n, 1, 128), f32),
                dma((4,)),
                dma((2, 3)),
                dma((3 + side,)),
                dma((2, 2, side)),
                dma((2, side, 3)),
                dma((2, 3, 3)),
                dma(()),
                dma((3,)),
                dma((3,)),
                dma((3,)),
                dma((3,)),
                dma((3,)),
                dma(()),
            ],
            compiler_params=pltpu.CompilerParams(collective_id=0, has_side_effects=True, vmem_limit_bytes=24 << 20),
        )(*(pltpu.with_memory_space_constraint(one, pltpu.HBM) for one in (*terms, *whole, *ms, *vs)))
        out = pl.pallas_call(
            write_out,
            out_shape=[jax.ShapeDtypeStruct(one.shape, one.dtype) for one in out],
            in_specs=[pl.BlockSpec(memory_space=pltpu.VMEM)] * 9,
            out_specs=[pl.BlockSpec(memory_space=pltpu.HBM)] * 9,
            scratch_shapes=[dma((9,))],
            compiler_params=pltpu.CompilerParams(vmem_limit_bytes=1 << 20),
        )(*out)
        return (*(one.reshape(w.shape) for one, w in zip(out[:3], weights, strict=True)), *out[3:])

    all_of, cut = P(None, None, None), P(None, "dp", None)
    return jax.shard_map(
        step,
        mesh=mesh,
        in_specs=(P(("rep", "dp"), None, None, None),) * 3 + (all_of,) * 3 + (cut,) * 6,
        out_specs=(P("rep", None, None),) * 3 + (P("rep", "dp", None),) * 6,
        check_vma=False,
    )
```

```python
import functools
import math

import jax
import jax.numpy as jnp
from jax import lax
from jax.experimental import pallas as pl
from jax.experimental.pallas import tpu as pltpu
from jax.sharding import PartitionSpec as P

CORES = 2
ROWS, COLS = 16, 512


def strips(shape):
    rows, cols = shape
    if rows > ROWS:
        return rows // ROWS, lambda i: (pl.ds(pl.multiple_of(i * ROWS, ROWS), ROWS), slice(None))
    return cols // COLS, lambda i: (slice(None), pl.ds(pl.multiple_of(i * COLS, COLS), COLS))


def kernel(n, side, *refs):
    (t, w, m, v, o, mo, vo, ring, pair, kept, g, held) = (refs[3 * i : 3 * i + 3] for i in range(12))
    (
        parts, own_sem, first_sem, mate_sem, ring_sem, late_sem, pair_sem, part_sem, state_sem, back_sem,
        mate_out, ring_out, pair_out, part_out, tail_sem, head_sem,
    ) = refs[36:]
    kinds, layers = range(3), range(2)
    f32, bf16 = jnp.float32, jnp.bfloat16

    me = lax.axis_index("dp")
    core, chip = lax.rem(me, CORES), lax.div(me, CORES)
    x, y = lax.div(chip, side), lax.rem(chip, side)
    a, b = x + core * (y - x), y + core * (x - y)
    mate = {"dp": me + 1 - 2 * core}

    def turn(i):
        return lax.rem(i + 2 * side, side)

    def place(a_, b_, core_=core):
        return a_ + core_ * (b_ - a_), b_ + core_ * (a_ - b_)

    def device(a_, b_):
        x_, y_ = place(a_, b_)
        return {"dp": (x_ * side + y_) * CORES + core}

    near_a = [device(turn(a - 1), b), device(turn(a + 1), b)]
    near_b = [device(a, turn(b + 1)), device(a, turn(b - 1))]

    def off(k):
        return 2 + k - 3 * (k // 2) - 2 * (k // 3)

    def role(d, s, k, a_, b_):
        step = 2 * d - 1
        to = turn(a_ + (0 if s == 3 else step + step * (s == 0)))
        return (1 - d if s == 1 else d), to, turn(b_ + off(k))

    def block(j, layer, a_, b_):
        return o[j].at[(layer, *place(a_, b_), core)]

    def other(j, layer, a_, b_):
        return o[j].at[(layer, *place(a_, b_), 1 - core)]

    def load(s, k):
        for d in layers:
            layer, a_, b_ = role(d, s, k, a, b)
            for j in kinds:
                pltpu.make_async_copy(t[j].at[(layer, *place(a_, b_), core)], block(j, layer, a_, b_), own_sem.at[s]).start()

    def for_mate(s, k):
        at = [role(d, s, k, b, a) for d in layers]
        for j in kinds:
            for d in layers:
                layer, to = at[d][0], place(*at[d][1:], 1 - core)
                yield d, j, t[j].at[(layer, *to, 1 - core)], o[j].at[(layer, *to, core)]

    def hand(s, k):
        for _, j, src, dst in for_mate(s, k):
            pltpu.make_async_remote_copy(src, dst, mate_out.at[j], mate_sem.at[3 + k if s == 0 else s - 1], device_id=mate).start()

    def arrived(ref, sem):
        pltpu.make_async_copy(ref, ref, sem).wait()

    def along_a(j, d, s, k):
        return late_sem.at[d, k, j] if s == 2 else ring_sem.at[d, s, k]

    def arrived_a(ref, j, d, s, k):
        if s == 2:
            arrived(ref, late_sem.at[d, k, j])
        elif j == 0:
            arrived(pair[0].at[0], ring_sem.at[d, s, k])

    def send(src, dst, out_sem, sem, to):
        pltpu.make_async_remote_copy(src, dst, out_sem, sem, device_id=to).start()

    def total(j, d, s, k, more=(), into=None):
        layer, a_, b_ = role(d, s, k, a, b)
        mine, its = block(j, layer, a_, b_), other(j, layer, a_, b_)
        into = mine if into is None else into
        count, cut = strips(mine.shape)

        @pl.loop(0, count, unroll=4)
        def _(i):
            at = cut(i)
            so_far = mine[at].astype(f32) + its[at].astype(f32)
            for one in more:
                so_far += one[at].astype(f32)
            into[at] = so_far.astype(into.dtype)

        return mine

    barrier = pltpu.get_barrier_semaphore()
    for to in (mate, *near_a, *near_b):
        pl.semaphore_signal(barrier, inc=1, device_id=to)
    pl.loop(0, side)(functools.partial(load, 0))
    pl.semaphore_wait(barrier, 5)

    for d, j, src, dst in for_mate(0, 0):
        send(src, dst, mate_out.at[j], first_sem.at[d, j], mate)
    pl.loop(1, side)(functools.partial(hand, 0))

    def out_along_a(s, k, first=False):
        if s == 0 and not first:
            arrived(pair[0], mate_sem.at[3 + k])
        for j in kinds:
            for d in layers:
                more = ()
                if first:
                    arrived(g[j].at[d], first_sem.at[d, j])
                if s == 2:
                    arrived_a(ring[j].at[d, 0, k], j, d, 0, k)
                    more = (ring[j].at[d, 0, k],)
                mine = total(j, d, s, k, more)
                send(mine, ring[j].at[d, s, k], ring_out.at[j], along_a(j, d, s, k), near_a[d])
        hand(s + 1, k)

    arrived(ring[0], own_sem.at[0])
    out_along_a(0, 0, True)
    for s in (1, 2, 3):
        pl.loop(0, side)(functools.partial(load, s))
    for j in kinds:
        x_, y_ = place(a, b)
        pltpu.make_async_copy(w[j].at[:, x_, y_, core], held[j], state_sem.at[0]).start()
        pltpu.make_async_copy(m[j], mo[j], state_sem.at[1]).start()
        pltpu.make_async_copy(v[j], vo[j], state_sem.at[2]).start()
    pl.loop(1, side)(functools.partial(out_along_a, 0))
    for s in (1, 2):
        arrived(ring[0], own_sem.at[s])
        arrived(ring[0], mate_sem.at[s - 1])
        pl.loop(0, side)(functools.partial(out_along_a, s))

    def last(j, layer, k, more=(), into=None):
        came = [ring[j].at[layer, 2, k], ring[j].at[1 - layer, 1, k]]
        arrived_a(came[0], j, layer, 2, k)
        arrived_a(came[1], j, 1 - layer, 1, k)
        return total(j, layer, 3, k, (*came, *more), into)

    arrived(ring[0], own_sem.at[3])
    arrived(ring[0], mate_sem.at[2])

    def onward(j, layer, k, d, s, more=()):
        send(last(j, layer, k, more), pair[j].at[d, s], pair_out.at[j], pair_sem.at[d, s, j], near_b[d])

    for j in kinds:
        for d in layers:
            onward(j, d, 0, d, 0)
    for j in kinds:
        onward(j, 0, 1, 1, 1)
        onward(j, 1, 2, 0, 1)
    for j in kinds:
        for layer, k, d in ((1, 1, 1), (0, 2, 0)):
            arrived(pair[j].at[d, 0], pair_sem.at[d, 0, j])
            onward(j, layer, k, d, 2, (pair[j].at[d, 0],))
    for j in kinds:
        for layer in layers:
            last(j, layer, 3, into=kept[j].at[layer])

    for j in kinds:
        arrived(o[j].at[:, :, :, 0], mate_out.at[j])
    squares = jnp.zeros((ROWS, COLS), f32)
    for j in kinds:
        for layer in layers:
            came = [pair[j].at[layer, 2], pair[j].at[1 - layer, 1]]
            arrived(came[0], pair_sem.at[layer, 2, j])
            arrived(came[1], pair_sem.at[1 - layer, 1, j])
            count, cut = strips(came[0].shape)

            def finish(i, so_far, j=j, layer=layer, came=came, cut=cut):
                at = cut(i)
                grad = kept[j].at[layer][at] + came[0][at].astype(f32) + came[1][at].astype(f32)
                grad = grad.astype(bf16)
                g[j].at[layer][at] = grad
                grad = grad.astype(f32)
                return so_far + grad * grad

            squares = lax.fori_loop(0, count, finish, squares, unroll=4)
    by_lane = jnp.sum(squares, axis=0, keepdims=True)
    parts[me] = sum(by_lane[:, i * 128 : (i + 1) * 128] for i in range(COLS // 128))
    for j in kinds:
        arrived(ring[j], ring_out.at[j])
        arrived(pair[j], pair_out.at[j])

    @pl.loop(1, n, unroll=True)
    def _(i):
        send(parts.at[me], parts.at[me], part_out, part_sem, {"dp": lax.rem(me + i, n)})

    arrived(pair[0], state_sem.at[0])
    arrived(ring[0].at[0], state_sem.at[1])
    arrived(ring[0].at[0], state_sem.at[2])
    arrived(parts.at[pl.ds(0, n - 1)], part_sem)
    count = n * sum(math.prod(one.shape) for one in mo)
    whole = jnp.sum(jnp.sum(parts[...], axis=0), axis=1, keepdims=True)
    factor = jnp.minimum(1.0, 0.5 * lax.rsqrt(whole / count + 1e-30))

    def pass_on(j, layer, a_, b_, *, on_a=(), on_b=()):
        one = block(j, layer, a_, b_)
        for d, s in on_b:
            send(one, one, pair_out.at[j], pair_sem.at[d, s, j], near_b[d])
        for d, s, k in on_a:
            send(one, one, ring_out.at[j], along_a(j, d, s, k), near_a[d])
        send(one, one, mate_out.at[j], back_sem.at[j], mate)

    for layer in layers:
        for j in kinds:
            new = block(j, layer, a, b)
            count, cut = strips(new.shape)

            @pl.loop(0, count, unroll=4)
            def _(i, j=j, layer=layer, new=new, cut=cut):
                at = cut(i)
                grad = g[j].at[layer][at].astype(f32) * factor
                m_ = 0.9 * mo[j].at[layer][at] + 0.1 * grad
                v_ = 0.95 * vo[j].at[layer][at] + 0.05 * grad * grad
                w_ = held[j].at[layer][at].astype(f32)
                mo[j].at[layer][at] = m_
                vo[j].at[layer][at] = v_
                new[at] = (w_ - 0.02 * (m_ * lax.rsqrt(v_ + 1e-8) + 0.1 * w_)).astype(bf16)

            pass_on(j, layer, a, b, on_a=[(d, layer, 3) for d in layers], on_b=[(d, layer) for d in layers])

    def from_b(j, d, s):
        layer = d if s == 2 else s
        step = 1 - 2 * d
        b_ = turn(b - (2 if s == 2 else 1) * step)
        k = 0 if s == 2 else 1 + d
        arrived(block(j, layer, a, b_), pair_sem.at[d, s, j])
        pass_on(j, layer, a, b_, on_a=[(e, layer, k) for e in layers], on_b=[(d, 2)] if s == d else [])

    def halves(one):
        rows = one.shape[0]
        part = rows * 5 // 8
        return one.at[pl.ds(0, part)], one.at[pl.ds(part, rows - part)]

    across_a = [{"dp": to["dp"] + 1 - 2 * core} for to in near_a]

    def from_a(j, d, s, k):
        layer = d if s == 2 else s
        step = 2 * d - 1
        a_, b_ = turn(a - (2 if s == 2 else 1) * step), turn(b + off(k))
        one = block(j, layer, a_, b_)
        is_last = (j, k) == (2, 0)
        if s == 2 and is_last:
            head, rest = halves(one)
            arrived(head, late_sem.at[d, k, j])
            send(head, head, ring_out.at[3], head_sem.at[d], mate)
            arrived(rest, tail_sem.at[d, 0])
            return
        arrived_a(one, j, d, s, k)
        pass_on(j, layer, a_, b_, on_a=[(d, 2, k)] if s == d and not is_last else [])
        if s == d and is_last:
            head, rest = halves(one)
            send(head, head, ring_out.at[j], late_sem.at[d, k, j], near_a[d])
            for other_core in (1 - core, core):
                to = {"dp": near_a[d]["dp"] + other_core * (across_a[d]["dp"] - near_a[d]["dp"])}
                send(rest, rest, ring_out.at[j + other_core], tail_sem.at[d, other_core], to)

    for j in kinds:
        from_b(j, 0, 0)
        from_b(j, 1, 1)
        from_a(j, 0, 0, 3)
        from_a(j, 1, 1, 3)
    for j in kinds:
        from_b(j, 0, 1)
        from_b(j, 1, 0)
    for j in kinds:
        from_b(j, 0, 2)
        from_b(j, 1, 2)
    for k in range(3):
        for j in kinds:
            from_a(j, 0, 0, (1, 2, 0)[k])
            from_a(j, 1, 1, (2, 1, 0)[k])
    for k in (3, 1, 2, 0):
        for j in kinds:
            from_a(j, 0, 1, k)
            from_a(j, 1, 0, k)
    for k in (3, 1, 2, 0):
        for j in kinds:
            from_a(j, 0, 2, k)
            from_a(j, 1, 2, k)

    for d in layers:
        head, rest = halves(block(2, d, a, b))
        arrived(head, head_sem.at[d])
        arrived(rest, tail_sem.at[d, 1])
    arrived(pair[2].at[0, pl.ds(0, 2)], ring_out.at[3])
    for j in kinds:
        half = o[j].at[:, :, :, 0]
        if j == 2:
            half = o[j].at[:, :, :, 0, pl.ds(0, half.shape[-2] * 15 // 16)]
        arrived(half, back_sem.at[j])
        arrived(half, mate_out.at[j])
        arrived(ring[j], ring_out.at[j])
        arrived(pair[j], pair_out.at[j])
    arrived(parts.at[pl.ds(0, n - 1)], part_out)


def write_out(*refs):
    sem = refs[-1]
    moves = [pltpu.make_async_copy(src, dst, sem.at[i]) for i, (src, dst) in enumerate(zip(refs[:9], refs[9:18], strict=True))]
    for one in moves:
        one.start()
    for one in moves:
        one.wait()


def solution(mesh):
    n = mesh.shape["dp"]
    side = math.isqrt(n // CORES)

    def step(*arrays):
        terms, weights, ms, vs = (arrays[i : i + 3] for i in (0, 3, 6, 9))
        blocks = [(one.shape[0], side, side, CORES, *one.shape[1:]) for one in ms]
        terms = [one.reshape(s) for one, s in zip(terms, blocks, strict=True)]
        whole = [one.reshape(s) for one, s in zip(weights, blocks, strict=True)]
        f32, bf16 = jnp.float32, jnp.bfloat16
        dma = pltpu.SemaphoreType.DMA
        tail = [s[-2:] for s in blocks]
        out = pl.pallas_call(
            functools.partial(kernel, n, side),
            out_shape=[pltpu.VMEM(s, bf16) for s in blocks] + [pltpu.VMEM(one.shape, f32) for one in (*ms, *vs)],
            in_specs=[pl.BlockSpec(memory_space=pltpu.HBM)] * 12,
            out_specs=[pl.BlockSpec(memory_space=pltpu.VMEM)] * 9,
            scratch_shapes=[
                *(pltpu.VMEM((2, 3, side, *s), bf16) for s in tail),
                *(pltpu.VMEM((2, 3, *s), bf16) for s in tail),
                *(pltpu.VMEM(one.shape, f32) for one in ms),
                *(pltpu.VMEM(one.shape, bf16) for one in ms),
                *(pltpu.VMEM(one.shape, bf16) for one in ms),
                pltpu.VMEM((n, 1, 128), f32),
                dma((4,)),
                dma((2, 3)),
                dma((3 + side,)),
                dma((2, 2, side)),
                dma((2, side, 3)),
                dma((2, 3, 3)),
                dma(()),
                dma((3,)),
                dma((3,)),
                dma((3,)),
                dma((4,)),
                dma((3,)),
                dma(()),
                dma((2, 2)),
                dma((2,)),
            ],
            compiler_params=pltpu.CompilerParams(collective_id=0, has_side_effects=True, vmem_limit_bytes=24 << 20),
        )(*(pltpu.with_memory_space_constraint(one, pltpu.HBM) for one in (*terms, *whole, *ms, *vs)))
        out = pl.pallas_call(
            write_out,
            out_shape=[jax.ShapeDtypeStruct(one.shape, one.dtype) for one in out],
            in_specs=[pl.BlockSpec(memory_space=pltpu.VMEM)] * 9,
            out_specs=[pl.BlockSpec(memory_space=pltpu.HBM)] * 9,
            scratch_shapes=[dma((9,))],
            compiler_params=pltpu.CompilerParams(vmem_limit_bytes=1 << 20),
        )(*out)
        return (*(one.reshape(w.shape) for one, w in zip(out[:3], weights, strict=True)), *out[3:])

    all_of, cut = P(None, None, None), P(None, "dp", None)
    return jax.shard_map(
        step,
        mesh=mesh,
        in_specs=(P(("rep", "dp"), None, None, None),) * 3 + (all_of,) * 3 + (cut,) * 6,
        out_specs=(P("rep", None, None),) * 3 + (P("rep", "dp", None),) * 6,
        check_vma=False,
    )
```

```python
import functools
import math

import jax
import jax.numpy as jnp
from jax import lax
from jax.experimental import pallas as pl
from jax.experimental.pallas import tpu as pltpu
from jax.sharding import PartitionSpec as P

CORES = 2
ROWS, COLS = 16, 512


def strips(shape):
    rows, cols = shape
    if rows > ROWS:
        return rows // ROWS, lambda i: (pl.ds(pl.multiple_of(i * ROWS, ROWS), ROWS), slice(None))
    return cols // COLS, lambda i: (slice(None), pl.ds(pl.multiple_of(i * COLS, COLS), COLS))


def kernel(n, side, *refs):
    (t, w, m, v, o, mo, vo, ring, pair, kept, g, held) = (refs[3 * i : 3 * i + 3] for i in range(12))
    (
        parts, own_sem, first_sem, mate_sem, ring_sem, late_sem, pair_sem, part_sem, state_sem,
        mate_out, ring_out, pair_out, part_out,
    ) = refs[36:]
    kinds, layers = range(3), range(2)
    f32, bf16 = jnp.float32, jnp.bfloat16

    me = lax.axis_index("dp")
    core, chip = lax.rem(me, CORES), lax.div(me, CORES)
    x, y = lax.div(chip, side), lax.rem(chip, side)
    a, b = x + core * (y - x), y + core * (x - y)
    mate = {"dp": me + 1 - 2 * core}

    def turn(i):
        return lax.rem(i + 2 * side, side)

    def place(a_, b_, core_=core):
        return a_ + core_ * (b_ - a_), b_ + core_ * (a_ - b_)

    def device(a_, b_):
        x_, y_ = place(a_, b_)
        return {"dp": (x_ * side + y_) * CORES + core}

    near_a = [device(turn(a - 1), b), device(turn(a + 1), b)]
    near_b = [device(a, turn(b + 1)), device(a, turn(b - 1))]

    def off(k):
        return 2 + k - 3 * (k // 2) - 2 * (k // 3)

    def role(d, s, k, a_, b_):
        step = 2 * d - 1
        to = turn(a_ + (0 if s == 3 else step + step * (s == 0)))
        return (1 - d if s == 1 else d), to, turn(b_ + off(k))

    def block(j, layer, a_, b_):
        return o[j].at[(layer, *place(a_, b_), core)]

    def other(j, layer, a_, b_):
        return o[j].at[(layer, *place(a_, b_), 1 - core)]

    def load(s, k):
        for d in layers:
            layer, a_, b_ = role(d, s, k, a, b)
            for j in kinds:
                pltpu.make_async_copy(t[j].at[(layer, *place(a_, b_), core)], block(j, layer, a_, b_), own_sem.at[s]).start()

    def for_mate(s, k):
        at = [role(d, s, k, b, a) for d in layers]
        for j in kinds:
            for d in layers:
                layer, to = at[d][0], place(*at[d][1:], 1 - core)
                yield d, j, t[j].at[(layer, *to, 1 - core)], o[j].at[(layer, *to, core)]

    def hand(s, k):
        for _, j, src, dst in for_mate(s, k):
            pltpu.make_async_remote_copy(src, dst, mate_out.at[j], mate_sem.at[2 + k if s == 0 else s - 1], device_id=mate).start()

    def arrived(ref, sem):
        pltpu.make_async_copy(ref, ref, sem).wait()

    def along_a(j, d, s, k):
        return late_sem.at[d, k, j] if s == 2 else ring_sem.at[d, s, k]

    def arrived_a(ref, j, d, s, k):
        if s == 2:
            arrived(ref, late_sem.at[d, k, j])
        elif j == 0:
            arrived(pair[0].at[0], ring_sem.at[d, s, k])

    def send(src, dst, out_sem, sem, to):
        pltpu.make_async_remote_copy(src, dst, out_sem, sem, device_id=to).start()

    def total(j, d, s, k, more=(), into=None):
        layer, a_, b_ = role(d, s, k, a, b)
        mine, its = block(j, layer, a_, b_), other(j, layer, a_, b_)
        into = mine if into is None else into
        count, cut = strips(mine.shape)

        @pl.loop(0, count, unroll=4)
        def _(i):
            at = cut(i)
            so_far = mine[at].astype(f32) + its[at].astype(f32)
            for one in more:
                so_far += one[at].astype(f32)
            into[at] = so_far.astype(into.dtype)

        return mine

    barrier = pltpu.get_barrier_semaphore()
    for to in (mate, *near_a, *near_b):
        pl.semaphore_signal(barrier, inc=1, device_id=to)
    pl.loop(0, side)(functools.partial(load, 0))
    pl.semaphore_wait(barrier, 5)

    for d, j, src, dst in for_mate(0, 0):
        send(src, dst, mate_out.at[j], first_sem.at[d, j], mate)
    pl.loop(1, side)(functools.partial(hand, 0))

    def out_along_a(s, k, first=False):
        if s == 0 and not first:
            arrived(pair[0], mate_sem.at[2 + k])
        for j in kinds:
            for d in layers:
                more = ()
                if first:
                    arrived(g[j].at[d], first_sem.at[d, j])
                if s == 2:
                    arrived_a(ring[j].at[d, 0, k], j, d, 0, k)
                    more = (ring[j].at[d, 0, k],)
                mine = total(j, d, s, k, more)
                send(mine, ring[j].at[d, s, k], ring_out.at[j], along_a(j, d, s, k), near_a[d])
        hand(s + 1, k)

    arrived(ring[0], own_sem.at[0])
    out_along_a(0, 0, True)
    for s in (1, 2, 3):
        pl.loop(0, side)(functools.partial(load, s))
    for j in kinds:
        x_, y_ = place(a, b)
        pltpu.make_async_copy(w[j].at[:, x_, y_, core], held[j], state_sem.at[0]).start()
        pltpu.make_async_copy(m[j], mo[j], state_sem.at[1]).start()
        pltpu.make_async_copy(v[j], vo[j], state_sem.at[2]).start()
    pl.loop(1, side)(functools.partial(out_along_a, 0))
    for s in (1, 2):
        arrived(ring[0], own_sem.at[s])
        arrived(ring[0], mate_sem.at[s - 1])
        pl.loop(0, side)(functools.partial(out_along_a, s))

    def last(j, layer, k, more=(), into=None):
        came = [ring[j].at[layer, 2, k], ring[j].at[1 - layer, 1, k]]
        arrived_a(came[0], j, layer, 2, k)
        arrived_a(came[1], j, 1 - layer, 1, k)
        return total(j, layer, 3, k, (*came, *more), into)

    arrived(ring[0], own_sem.at[3])
    arrived(ring[0], mate_sem.at[2])

    def onward(j, layer, k, d, s, more=()):
        send(last(j, layer, k, more), pair[j].at[d, s], pair_out.at[j], pair_sem.at[d, s, j], near_b[d])

    for j in kinds:
        for d in layers:
            onward(j, d, 0, d, 0)
    for j in kinds:
        onward(j, 0, 1, 1, 1)
        onward(j, 1, 2, 0, 1)
    for j in kinds:
        for layer, k, d in ((1, 1, 1), (0, 2, 0)):
            arrived(pair[j].at[d, 0], pair_sem.at[d, 0, j])
            onward(j, layer, k, d, 2, (pair[j].at[d, 0],))
    for j in kinds:
        for layer in layers:
            last(j, layer, 3, into=kept[j].at[layer])

    for j in kinds:
        arrived(o[j].at[:, :, :, 0], mate_out.at[j])
    squares = jnp.zeros((ROWS, COLS), f32)
    for j in kinds:
        for layer in layers:
            came = [pair[j].at[layer, 2], pair[j].at[1 - layer, 1]]
            arrived(came[0], pair_sem.at[layer, 2, j])
            arrived(came[1], pair_sem.at[1 - layer, 1, j])
            count, cut = strips(came[0].shape)

            def finish(i, so_far, j=j, layer=layer, came=came, cut=cut):
                at = cut(i)
                grad = kept[j].at[layer][at] + came[0][at].astype(f32) + came[1][at].astype(f32)
                grad = grad.astype(bf16)
                g[j].at[layer][at] = grad
                grad = grad.astype(f32)
                return so_far + grad * grad

            squares = lax.fori_loop(0, count, finish, squares, unroll=4)
    by_lane = jnp.sum(squares, axis=0, keepdims=True)
    parts[me] = sum(by_lane[:, i * 128 : (i + 1) * 128] for i in range(COLS // 128))
    for j in kinds:
        arrived(ring[j], ring_out.at[j])
        arrived(pair[j], pair_out.at[j])

    @pl.loop(1, n, unroll=True)
    def _(i):
        send(parts.at[me], parts.at[me], part_out, part_sem, {"dp": lax.rem(me + i, n)})

    arrived(pair[0], state_sem.at[0])
    arrived(ring[0].at[0], state_sem.at[1])
    arrived(ring[0].at[0], state_sem.at[2])
    arrived(parts.at[pl.ds(0, n - 1)], part_sem)
    count = n * sum(math.prod(one.shape) for one in mo)
    whole = jnp.sum(jnp.sum(parts[...], axis=0), axis=1, keepdims=True)
    factor = jnp.minimum(1.0, 0.5 * lax.rsqrt(whole / count + 1e-30))

    def pass_on(j, layer, a_, b_, *, on_a=(), on_b=()):
        one = block(j, layer, a_, b_)
        for d, s in on_b:
            send(one, one, pair_out.at[j], pair_sem.at[d, s, j], near_b[d])
        for d, s, k in on_a:
            send(one, one, ring_out.at[j], along_a(j, d, s, k), near_a[d])
        send(one, one, mate_out.at[j], own_sem.at[j], mate)

    for layer in layers:
        for j in kinds:
            new = block(j, layer, a, b)
            count, cut = strips(new.shape)

            @pl.loop(0, count, unroll=8)
            def _(i, j=j, layer=layer, new=new, cut=cut):
                at = cut(i)
                grad = g[j].at[layer][at].astype(f32) * factor
                m_ = 0.9 * mo[j].at[layer][at] + 0.1 * grad
                v_ = 0.95 * vo[j].at[layer][at] + 0.05 * grad * grad
                w_ = held[j].at[layer][at].astype(f32)
                mo[j].at[layer][at] = m_
                vo[j].at[layer][at] = v_
                new[at] = (w_ - 0.02 * (m_ * lax.rsqrt(v_ + 1e-8) + 0.1 * w_)).astype(bf16)

            pass_on(j, layer, a, b, on_a=[(d, layer, 3) for d in layers], on_b=[(d, layer) for d in layers])

    def from_b(j, d, s):
        layer = d if s == 2 else s
        step = 1 - 2 * d
        b_ = turn(b - (2 if s == 2 else 1) * step)
        k = 0 if s == 2 else 1 + d
        arrived(block(j, layer, a, b_), pair_sem.at[d, s, j])
        pass_on(j, layer, a, b_, on_a=[(e, layer, k) for e in layers], on_b=[(d, 2)] if s == d else [])

    def halves(one):
        rows = one.shape[0]
        part = rows * 5 // 8
        return one.at[pl.ds(0, part)], one.at[pl.ds(part, rows - part)]

    across_a = [{"dp": to["dp"] + 1 - 2 * core} for to in near_a]

    def from_a(j, d, s, k):
        layer = d if s == 2 else s
        step = 2 * d - 1
        a_, b_ = turn(a - (2 if s == 2 else 1) * step), turn(b + off(k))
        one = block(j, layer, a_, b_)
        is_last = (j, k) == (2, 0)
        if s == 2 and is_last:
            head, rest = halves(one)
            arrived(head, late_sem.at[d, k, j])
            send(head, head, ring_out.at[3], first_sem.at[d, 2], mate)
            arrived(rest, first_sem.at[d, 0])
            return
        arrived_a(one, j, d, s, k)
        pass_on(j, layer, a_, b_, on_a=[(d, 2, k)] if s == d and not is_last else [])
        if s == d and is_last:
            head, rest = halves(one)
            send(head, head, ring_out.at[j], late_sem.at[d, k, j], near_a[d])
            for other_core in (1 - core, core):
                to = {"dp": near_a[d]["dp"] + other_core * (across_a[d]["dp"] - near_a[d]["dp"])}
                send(rest, rest, ring_out.at[j + other_core], first_sem.at[d, other_core], to)

    for j in kinds:
        from_b(j, 0, 0)
        from_b(j, 1, 1)
        from_a(j, 0, 0, 3)
        from_a(j, 1, 1, 3)
    for j in kinds:
        from_b(j, 0, 1)
        from_b(j, 1, 0)
    for j in kinds:
        from_b(j, 0, 2)
        from_b(j, 1, 2)
    for k in range(3):
        for j in kinds:
            from_a(j, 0, 0, (1, 2, 0)[k])
            from_a(j, 1, 1, (2, 1, 0)[k])
    for k in (3, 1, 2, 0):
        for j in kinds:
            from_a(j, 0, 1, k)
            from_a(j, 1, 0, k)
    for k in (3, 1, 2, 0):
        for j in kinds:
            from_a(j, 0, 2, k)
            from_a(j, 1, 2, k)

    for d in layers:
        head, rest = halves(block(2, d, a, b))
        arrived(head, first_sem.at[d, 2])
        arrived(rest, first_sem.at[d, 1])
    arrived(pair[2].at[0, pl.ds(0, 2)], ring_out.at[3])
    for j in kinds:
        half = o[j].at[:, :, :, 0]
        if j == 2:
            half = o[j].at[:, :, :, 0, pl.ds(0, half.shape[-2] * 15 // 16)]
        arrived(half, own_sem.at[j])
        arrived(half, mate_out.at[j])
        arrived(ring[j], ring_out.at[j])
        arrived(pair[j], pair_out.at[j])
    arrived(parts.at[pl.ds(0, n - 1)], part_out)


def write_out(*refs):
    sem = refs[-1]
    moves = [pltpu.make_async_copy(src, dst, sem.at[i]) for i, (src, dst) in enumerate(zip(refs[:9], refs[9:18], strict=True))]
    for one in moves:
        one.start()
    for one in moves:
        one.wait()


def solution(mesh):
    n = mesh.shape["dp"]
    side = math.isqrt(n // CORES)

    def step(*arrays):
        terms, weights, ms, vs = (arrays[i : i + 3] for i in (0, 3, 6, 9))
        blocks = [(one.shape[0], side, side, CORES, *one.shape[1:]) for one in ms]
        terms = [one.reshape(s) for one, s in zip(terms, blocks, strict=True)]
        whole = [one.reshape(s) for one, s in zip(weights, blocks, strict=True)]
        f32, bf16 = jnp.float32, jnp.bfloat16
        dma = pltpu.SemaphoreType.DMA
        tail = [s[-2:] for s in blocks]
        out = pl.pallas_call(
            functools.partial(kernel, n, side),
            out_shape=[pltpu.VMEM(s, bf16) for s in blocks] + [pltpu.VMEM(one.shape, f32) for one in (*ms, *vs)],
            in_specs=[pl.BlockSpec(memory_space=pltpu.HBM)] * 12,
            out_specs=[pl.BlockSpec(memory_space=pltpu.VMEM)] * 9,
            scratch_shapes=[
                *(pltpu.VMEM((2, 3, side, *s), bf16) for s in tail),
                *(pltpu.VMEM((2, 3, *s), bf16) for s in tail),
                *(pltpu.VMEM(one.shape, f32) for one in ms),
                *(pltpu.VMEM(one.shape, bf16) for one in ms),
                *(pltpu.VMEM(one.shape, bf16) for one in ms),
                pltpu.VMEM((n, 1, 128), f32),
                dma((4,)),
                dma((2, 3)),
                dma((2 + side,)),
                dma((2, 2, side)),
                dma((2, side, 3)),
                dma((2, 3, 3)),
                dma(()),
                dma((3,)),
                dma((3,)),
                dma((4,)),
                dma((3,)),
                dma(()),
            ],
            compiler_params=pltpu.CompilerParams(collective_id=0, has_side_effects=True, vmem_limit_bytes=24 << 20),
        )(*(pltpu.with_memory_space_constraint(one, pltpu.HBM) for one in (*terms, *whole, *ms, *vs)))
        out = pl.pallas_call(
            write_out,
            out_shape=[jax.ShapeDtypeStruct(one.shape, one.dtype) for one in out],
            in_specs=[pl.BlockSpec(memory_space=pltpu.VMEM)] * 9,
            out_specs=[pl.BlockSpec(memory_space=pltpu.HBM)] * 9,
            scratch_shapes=[dma((9,))],
            compiler_params=pltpu.CompilerParams(vmem_limit_bytes=1 << 20),
        )(*out)
        return (*(one.reshape(w.shape) for one, w in zip(out[:3], weights, strict=True)), *out[3:])

    all_of, cut = P(None, None, None), P(None, "dp", None)
    return jax.shard_map(
        step,
        mesh=mesh,
        in_specs=(P(("rep", "dp"), None, None, None),) * 3 + (all_of,) * 3 + (cut,) * 6,
        out_specs=(P("rep", None, None),) * 3 + (P("rep", "dp", None),) * 6,
        check_vma=False,
    )
```
